32 devices in a mesh: dp: 1 (over z), tp: 4 (over y), fsdp: 4 (over x), cp: 2 (over core).
Axes of the slice: x: 4, y: 4, z: 1, core: 2. Of those that a mesh axis runs over, the one named last changes fastest.
The devices are a block of a 4x4x8 slice.
Arguments:
- hidden: bfloat16 [12, 1536, 4096], P(('dp', 'fsdp'), 'cp')
- positions: int32 [12, 1536], P(('dp', 'fsdp'), 'cp')
- attn_gain: float32 [4096], replicated
- w_query: bfloat16 [4096, 32, 128], P(('fsdp', 'cp'), 'tp')
- w_key: bfloat16 [4096, 8, 128], P(('fsdp', 'cp'), 'tp')
- w_value: bfloat16 [4096, 8, 128], P(('fsdp', 'cp'), 'tp')
- w_out: bfloat16 [32, 128, 4096], P('tp', None, ('fsdp', 'cp'))
- mlp_gain: float32 [4096], replicated
- w_gate: bfloat16 [4096, 14336], P(('fsdp', 'cp'), 'tp')
- w_up: bfloat16 [4096, 14336], P(('fsdp', 'cp'), 'tp')
- w_down: bfloat16 [14336, 4096], P('tp', ('fsdp', 'cp'))
Outputs:
- output: bfloat16 [12, 1536, 4096], P(('dp', 'fsdp'), 'cp')
All inputs are finite; a program needn't handle non-finite values.
Results may differ from the reference program's by a relative error of at most 0.0135401.
Values are sent between devices in bfloat16 or wider.
A program may use at most 768 MiB of HBM per device.

```python
import numpy as np
import jax
import jax.numpy as jnp
from jax import lax

SEQS = 3
SEG_LEN = 384
CP = 2
FSDP = 4
D = 4096
HEADS = 32
KV_HEADS = 8
HEAD = 128
FF = 14336
QBLOCK = 128
ROPE_THETA = 500000.0
NORM_EPS = 1e-5
BATCH = FSDP * SEQS
SEQ = 2 * CP * SEG_LEN
GROUP = HEADS // KV_HEADS


def setup_inputs(seed: int = 0, part: int = 0) -> dict:
    part_keys = jax.random.split(jax.random.fold_in(jax.random.key(seed), part), 3)
    weight_keys = jax.random.split(jax.random.key(seed + 7919), 9)
    noise = jax.random.normal(part_keys[0], (BATCH, 2 * CP, SEG_LEN, D), jnp.float32)
    seg_mean = jax.random.normal(part_keys[1], (BATCH, 2 * CP, 1, D), jnp.float32)
    hidden = (0.6 * noise + seg_mean).reshape(BATCH, SEQ, D).astype(jnp.bfloat16)
    gaps = jax.random.randint(part_keys[2], (BATCH, SEQ), 1, 5, dtype=jnp.int32)
    true_pos = jnp.cumsum(gaps, axis=1) - 1
    seg_order = np.array([slot // 2 if slot % 2 == 0 else 2 * CP - 1 - slot // 2 for slot in range(2 * CP)])
    positions = true_pos.reshape(BATCH, 2 * CP, SEG_LEN)[:, seg_order].reshape(BATCH, SEQ).astype(jnp.int32)
    in_scale = D ** -0.5
    return {
        'hidden': hidden,
        'positions': positions,
        'attn_gain': 1.0 + 0.25 * jax.random.normal(weight_keys[0], (D,), jnp.float32),
        'w_query': (1.5 * in_scale * jax.random.normal(weight_keys[1], (D, HEADS, HEAD), jnp.float32)).astype(jnp.bfloat16),
        'w_key': (1.5 * in_scale * jax.random.normal(weight_keys[2], (D, KV_HEADS, HEAD), jnp.float32)).astype(jnp.bfloat16),
        'w_value': (in_scale * jax.random.normal(weight_keys[3], (D, KV_HEADS, HEAD), jnp.float32)).astype(jnp.bfloat16),
        'w_out': ((HEADS * HEAD) ** -0.5 * jax.random.normal(weight_keys[4], (HEADS, HEAD, D), jnp.float32)).astype(jnp.bfloat16),
        'mlp_gain': 1.0 + 0.25 * jax.random.normal(weight_keys[5], (D,), jnp.float32),
        'w_gate': (in_scale * jax.random.normal(weight_keys[6], (D, FF), jnp.float32)).astype(jnp.bfloat16),
        'w_up': (in_scale * jax.random.normal(weight_keys[7], (D, FF), jnp.float32)).astype(jnp.bfloat16),
        'w_down': (FF ** -0.5 * jax.random.normal(weight_keys[8], (FF, D), jnp.float32)).astype(jnp.bfloat16),
    }


def rms_norm(hidden_f32, gain):
    mean_sq = jnp.mean(hidden_f32 * hidden_f32, axis=-1, keepdims=True)
    return (hidden_f32 * lax.rsqrt(mean_sq + NORM_EPS) * gain).astype(jnp.bfloat16)


def rope_tables(positions):
    inv_freq = ROPE_THETA ** (-jnp.arange(0, HEAD, 2, dtype=jnp.float32) / HEAD)
    angles = positions.astype(jnp.float32)[..., None] * inv_freq
    return jnp.cos(angles)[..., None, :], jnp.sin(angles)[..., None, :]


def apply_rope(projected, rope_cos, rope_sin):
    half_dim = projected.shape[-1] // 2
    first_half = projected[..., :half_dim]
    second_half = projected[..., half_dim:]
    return jnp.concatenate([first_half * rope_cos - second_half * rope_sin, second_half * rope_cos + first_half * rope_sin], axis=-1)


def attention(queries, keys, values, positions):
    n_blocks = SEQ // QBLOCK
    q_blocks = queries.reshape(BATCH * n_blocks, QBLOCK, KV_HEADS, GROUP, HEAD)
    pos_blocks = positions.reshape(BATCH * n_blocks, QBLOCK)
    seq_ids = jnp.arange(BATCH * n_blocks) // n_blocks
    keys_f32 = keys.astype(jnp.float32)
    values_f32 = values.astype(jnp.float32)

    def one_block(block_args):
        q_blk, qpos_blk, seq_id = block_args
        k_seq = lax.dynamic_index_in_dim(keys_f32, seq_id, 0, keepdims=False)
        v_seq = lax.dynamic_index_in_dim(values_f32, seq_id, 0, keepdims=False)
        kpos_seq = lax.dynamic_index_in_dim(positions, seq_id, 0, keepdims=False)
        scores = jnp.einsum('qkgd,skd->kgqs', q_blk.astype(jnp.float32), k_seq) * (HEAD ** -0.5)
        visible = qpos_blk[:, None] >= kpos_seq[None, :]
        scores = jnp.where(visible, scores, -jnp.inf)
        row_max = jnp.max(scores, axis=-1, keepdims=True)
        probs = jnp.exp(scores - row_max)
        row_sum = jnp.sum(probs, axis=-1)
        weighted = jnp.einsum('kgqs,skd->qkgd', probs.astype(jnp.bfloat16).astype(jnp.float32), v_seq)
        return (weighted / jnp.transpose(row_sum, (2, 0, 1))[..., None]).astype(jnp.bfloat16)

    mixed = lax.map(one_block, (q_blocks, pos_blocks, seq_ids))
    return mixed.reshape(BATCH, SEQ, HEADS, HEAD)


def reference(hidden, positions, attn_gain, w_query, w_key, w_value, w_out, mlp_gain, w_gate, w_up, w_down):
    hidden_f32 = hidden.astype(jnp.float32)
    normed = rms_norm(hidden_f32, attn_gain).astype(jnp.float32)
    rope_cos, rope_sin = rope_tables(positions)
    queries = apply_rope(jnp.einsum('bsd,dhe->bshe', normed, w_query.astype(jnp.float32)), rope_cos, rope_sin).astype(jnp.bfloat16)
    keys = apply_rope(jnp.einsum('bsd,dhe->bshe', normed, w_key.astype(jnp.float32)), rope_cos, rope_sin).astype(jnp.bfloat16)
    values = jnp.einsum('bsd,dhe->bshe', normed, w_value.astype(jnp.float32)).astype(jnp.bfloat16)
    mixed = attention(queries.reshape(BATCH, SEQ, KV_HEADS, GROUP, HEAD), keys, values, positions)
    attn_out = jnp.einsum('bshe,hed->bsd', mixed.astype(jnp.float32), w_out.astype(jnp.float32)).astype(jnp.bfloat16)
    mid_resid = (hidden_f32 + attn_out.astype(jnp.float32)).astype(jnp.bfloat16)
    mid_f32 = mid_resid.astype(jnp.float32)
    normed_mlp = rms_norm(mid_f32, mlp_gain).astype(jnp.float32)
    gate_proj = jnp.einsum('bsd,df->bsf', normed_mlp, w_gate.astype(jnp.float32))
    up_proj = jnp.einsum('bsd,df->bsf', normed_mlp, w_up.astype(jnp.float32))
    act_mlp = (jax.nn.silu(gate_proj) * up_proj).astype(jnp.bfloat16)
    down_proj = jnp.einsum('bsf,fd->bsd', act_mlp.astype(jnp.float32), w_down.astype(jnp.float32)).astype(jnp.bfloat16)
    return (mid_f32 + down_proj.astype(jnp.float32)).astype(jnp.bfloat16)
```

```python
import functools
import math

import jax
import jax.numpy as jnp
from jax import lax
from jax.experimental import pallas as pl
from jax.experimental.pallas import tpu as pltpu
from jax.sharding import PartitionSpec as P


ROPE_THETA = 500000.0
NORM_EPS = 1e-5
GROUP_AXES = ('fsdp', 'cp')
VMEM_LIMIT = 62 * 1024 * 1024
F32 = jnp.float32
BF16 = jnp.bfloat16
MESH = pl.DeviceIdType.MESH
ANY = pl.BlockSpec(memory_space=pl.ANY)
VMEM = pl.BlockSpec(memory_space=pltpu.VMEM)


def rms_norm(hidden_f32, gain):
    mean_sq = jnp.mean(hidden_f32 * hidden_f32, axis=-1, keepdims=True)
    return (hidden_f32 * lax.rsqrt(mean_sq + NORM_EPS) * gain).astype(BF16)


def cost(flops, bytes_accessed):
    return pl.CostEstimate(flops=int(flops), bytes_accessed=int(bytes_accessed), transcendentals=0)


def proj_kernel(rope_heads, head, x_ref, w_ref, cos_ref, sin_ref, o_ref):
    acc = jnp.dot(x_ref[...], w_ref[...], preferred_element_type=F32)
    cos, sin = cos_ref[...], sin_ref[...]
    for i in range(acc.shape[1] // head):
        part = acc[:, i * head:(i + 1) * head]
        if i < rope_heads:
            part = part * cos + pltpu.roll(part, head // 2, 1) * sin
        o_ref[:, i * head:(i + 1) * head] = part.astype(BF16)


def project(x, w, cos, sin, col_block, width, rope_heads, head, tile=256):
    rows, depth = x.shape
    tile = math.gcd(tile, rows)
    return pl.pallas_call(
        functools.partial(proj_kernel, rope_heads, head),
        grid=(rows // tile,),
        in_specs=[
            pl.BlockSpec((tile, depth), lambda i: (i, 0)),
            pl.BlockSpec((depth, width), lambda i: (0, col_block)),
            pl.BlockSpec((tile, head), lambda i: (i, 0)),
            pl.BlockSpec((tile, head), lambda i: (i, 0)),
        ],
        out_specs=pl.BlockSpec((tile, width), lambda i: (i, 0)),
        out_shape=jax.ShapeDtypeStruct((rows, width), BF16),
        compiler_params=pltpu.CompilerParams(vmem_limit_bytes=VMEM_LIMIT),
        cost_estimate=cost(2 * rows * depth * width, 2 * (rows * depth + depth * width + rows * width)),
    )(x, w, cos, sin)


def attn_kernel(group, head, seg, q_ref, ko_ref, vo_ref, kp_ref, vp_ref, o_ref):
    c = lax.axis_index('cp')
    scale = head ** -0.5 * math.log2(math.e)

    def run(first_full, second_full):
        low, high = pl.ds(0, seg), pl.ds(seg, seg)
        own_low, own_high = (ko_ref, vo_ref, low), (ko_ref, vo_ref, high)
        tri = lax.broadcasted_iota(jnp.int32, (seg, seg), 0) >= lax.broadcasted_iota(jnp.int32, (seg, seg), 1)
        for g in range(group):
            cols = pl.ds(g * head, head)
            for rows, diag, full in ((low, own_low, first_full), (high, own_high, second_full)):
                q = q_ref[rows, cols]
                blocks = full + [diag]
                scores = []
                for k_ref, _, part in blocks:
                    scores.append(lax.dot_general(q, k_ref[part, :], (((1,), (1,)), ((), ())), preferred_element_type=F32))
                scores[-1] = jnp.where(tri, scores[-1], -jnp.inf)
                top = functools.reduce(jnp.maximum, [jnp.max(s, axis=-1, keepdims=True) for s in scores])
                total = jnp.zeros((seg, 1), F32)
                out = jnp.zeros((seg, head), F32)
                for s, (_, v_ref, part) in zip(scores, blocks):
                    p = jnp.exp2((s - top) * scale)
                    total = total + jnp.sum(p, axis=-1, keepdims=True)
                    out = out + jnp.dot(p.astype(BF16), v_ref[part, :], preferred_element_type=F32)
                o_ref[rows, cols] = (out / total).astype(BF16)

    low, high = pl.ds(0, seg), pl.ds(seg, seg)
    own_low, peer_low, peer_high = (ko_ref, vo_ref, low), (kp_ref, vp_ref, low), (kp_ref, vp_ref, high)

    @pl.when(c == 0)
    def _():
        run([], [own_low, peer_low, peer_high])

    @pl.when(c == 1)
    def _():
        run([peer_low], [peer_low, own_low])


def attention(q, kv_own, kv_peer, n_seqs, kv_heads, group, head):
    rows = q.shape[0]
    tokens = rows // n_seqs
    q_spec = pl.BlockSpec((tokens, group * head), lambda i, h: (i, h))
    k_spec = pl.BlockSpec((tokens, head), lambda i, h: (i, h))
    v_spec = pl.BlockSpec((tokens, head), lambda i, h: (i, kv_heads + h))
    return pl.pallas_call(
        functools.partial(attn_kernel, group, head, tokens // 2),
        grid=(n_seqs, kv_heads),
        in_specs=[q_spec, k_spec, v_spec, k_spec, v_spec],
        out_specs=q_spec,
        out_shape=jax.ShapeDtypeStruct(q.shape, BF16),
        compiler_params=pltpu.CompilerParams(vmem_limit_bytes=VMEM_LIMIT),
        cost_estimate=cost(10 * rows * tokens * kv_heads * group * head, 4 * q.size),
    )(q, kv_own, kv_own, kv_peer, kv_peer)


def ring_barrier(right, left):
    barrier = pltpu.get_barrier_semaphore()
    for neighbour in (right, left):
        pl.semaphore_signal(barrier, inc=1, device_id={'tp': neighbour}, device_id_type=MESH)
    pl.semaphore_wait(barrier, 2)


def ring_place(n):
    me = lax.axis_index('tp')
    return me, lax.rem(me + 1, n), lax.rem(me + n - 1, n)


def shard_of(me, direction, back, n):
    return lax.rem(me + (n - back if direction == 0 else back), n)


def ring_matmul_scatter(n, me, sides, u_refs, w_ref, u_buf, w_buf, s_buf, r_buf, u_sem, w_sem, send_sem, recv_sem, finish):
    half = u_buf.shape[2]
    block = w_buf.shape[2]
    blocks = w_ref.shape[1] // block

    def u_copies(step):
        copies = []
        for d in range(2):
            row = pl.multiple_of(shard_of(me, d, step + 1, n) * (2 * half) + d * half, 16)
            at = 0
            for i, u_ref in enumerate(u_refs):
                copies.append(pltpu.make_async_copy(
                    u_ref.at[pl.ds(row, half), :], u_buf.at[step % 2, d, :, pl.ds(at, u_ref.shape[1])], u_sem.at[step % 2, d, i]))
                at += u_ref.shape[1]
        return copies

    def w_copy(cb, slot):
        return pltpu.make_async_copy(w_ref.at[:, pl.ds(pl.multiple_of(cb * block, block), block)], w_buf.at[slot], w_sem.at[slot])

    def send(step, d, cb):
        src = s_buf.at[d, cb] if step == 0 else r_buf.at[step - 1, d, cb]
        return pltpu.make_async_remote_copy(
            src_ref=src, dst_ref=r_buf.at[step, d, cb], send_sem=send_sem.at[step, d, cb], recv_sem=recv_sem.at[step, d, cb],
            device_id={'tp': sides[d]}, device_id_type=MESH)

    for c in u_copies(0):
        c.start()
    w_copy(0, 0).start()
    for step in range(n):
        for c in u_copies(step):
            c.wait()
        if step + 1 < n:
            for c in u_copies(step + 1):
                c.start()

        def one_block(cb, _, step=step):
            slot = lax.rem(cb, 2)
            w_copy(cb, slot).wait()
            if step + 1 < n:
                w_copy(lax.rem(cb + 1, blocks), 1 - slot).start()
            else:
                @pl.when(cb + 1 < blocks)
                def _():
                    w_copy(cb + 1, 1 - slot).start()
            parts = [jnp.dot(u_buf[step % 2, d], w_buf[slot], preferred_element_type=F32) for d in range(2)]
            for d in range(2):
                part = parts[d]
                if step > 0:
                    send(step - 1, d, cb).wait_recv()
                    part = part + r_buf[step - 1, d, cb].astype(F32)
                if step + 1 < n:
                    if step == 0:
                        s_buf[d, cb] = part.astype(BF16)
                    else:
                        r_buf[step - 1, d, cb] = part.astype(BF16)
                    send(step, d, cb).start()
                else:
                    finish(d, cb, part)
            return 0

        lax.fori_loop(0, blocks, one_block, 0)

    def drain(cb, _):
        for step in range(n - 1):
            for d in range(2):
                send(step, d, cb).wait_send()
        return 0

    lax.fori_loop(0, blocks, drain, 0)


def ring_scratch(n, half, depth, block, blocks, n_u):
    return [
        pltpu.VMEM((2, 2, half, depth), BF16),
        pltpu.VMEM((2, depth, block), BF16),
        pltpu.VMEM((2, blocks, half, block), BF16),
        pltpu.VMEM((n - 1, 2, blocks, half, block), BF16),
        pltpu.SemaphoreType.DMA((2, 2, n_u)),
        pltpu.SemaphoreType.DMA((2,)),
        pltpu.SemaphoreType.DMA((n - 1, 2, blocks)),
        pltpu.SemaphoreType.DMA((n - 1, 2, blocks)),
    ]


def out_kernel(n, o_ref, w_ref, h_ref, gain_ref, r_ref, b_ref, h_buf, h_sem, u_buf, w_buf, s_buf, r_buf, u_sem, w_sem, send_sem, recv_sem):
    me, right, left = ring_place(n)
    shard, _ = r_ref.shape
    half = shard // 2
    block = w_buf.shape[2]
    load_h = pltpu.make_async_copy(h_ref.at[pl.ds(pl.multiple_of(me * shard, 16), shard), :], h_buf, h_sem)
    load_h.start()
    ring_barrier(right, left)
    load_h.wait()

    def finish(d, cb, part):
        rows, cols = pl.ds(d * half, half), pl.ds(pl.multiple_of(cb * block, block), block)
        total = h_buf[rows, cols].astype(F32) + part.astype(BF16).astype(F32)
        r_ref[rows, cols] = total.astype(BF16)

    ring_matmul_scatter(n, me, (right, left), [o_ref], w_ref, u_buf, w_buf, s_buf, r_buf, u_sem, w_sem, send_sem, recv_sem, finish)
    gain = gain_ref[...]

    def norm_rows(i, _):
        rows = pl.ds(pl.multiple_of(i * 16, 16), 16)
        b_ref[rows, :] = rms_norm(r_ref[rows, :].astype(F32), gain)
        return 0

    lax.fori_loop(0, shard // 16, norm_rows, 0)


def out_project(n, mixed, w_out, hidden, gain):
    rows, depth = mixed.shape
    width = w_out.shape[1]
    shard = rows // n
    block = min(512, width // 2)
    blocks = width // block
    return pl.pallas_call(
        functools.partial(out_kernel, n),
        in_specs=[ANY, ANY, ANY, VMEM],
        out_specs=[VMEM, VMEM],
        out_shape=[jax.ShapeDtypeStruct((shard, width), BF16)] * 2,
        scratch_shapes=[pltpu.VMEM((shard, width), BF16), pltpu.SemaphoreType.DMA]
        + ring_scratch(n, shard // 2, depth, block, blocks, 1),
        compiler_params=pltpu.CompilerParams(collective_id=0, has_side_effects=True, vmem_limit_bytes=VMEM_LIMIT),
        cost_estimate=cost(2 * rows * depth * width * 5, 2 * (rows * depth + depth * width)),
    )(mixed, w_out, hidden, gain)


def gated(x, w_gate, w_up):
    gate = jnp.dot(x, w_gate, preferred_element_type=F32)
    up = jnp.dot(x, w_up, preferred_element_type=F32)
    return (jax.nn.silu(gate) * up).astype(BF16)


def gather_gate_kernel(n, pieces, b_ref, w_ref, all_ref, u_ref, w_buf, x_buf, u_buf, w_sem, x_sem, own_sem, u_sem, send_sem, recv_sem):
    me, right, left = ring_place(n)
    sides = (right, left)
    shard = b_ref.shape[0]
    half = shard // 2
    piece = half // pieces
    ff = u_ref.shape[1]
    tile = min(256, ff)
    tiles = ff // tile

    def w_copies(t):
        out = []
        for i in range(2):
            cols = pl.ds(pl.multiple_of(i * ff + t * tile, tile), tile)
            out.append(pltpu.make_async_copy(w_ref.at[:, cols], w_buf.at[:, cols], w_sem.at[t, i]))
        return out

    def rows_of(d, back, j):
        return pl.ds(pl.multiple_of(shard_of(me, d, back, n) * shard + d * half + j * piece, 16), piece)

    def hop(a, d, j):
        rows = rows_of(d, a, j)
        src = b_ref.at[pl.ds(d * half + j * piece, piece), :] if a == 0 else all_ref.at[rows, :]
        return pltpu.make_async_remote_copy(
            src_ref=src, dst_ref=all_ref.at[rows, :], send_sem=send_sem.at[a, d, j], recv_sem=recv_sem.at[a, d, j],
            device_id={'tp': sides[d]}, device_id_type=MESH)

    def arrival(a, d, j):
        rows = rows_of(d, a + 1, j)
        return pltpu.make_async_remote_copy(
            src_ref=all_ref.at[rows, :], dst_ref=all_ref.at[rows, :], send_sem=send_sem.at[a, d, j], recv_sem=recv_sem.at[a, d, j],
            device_id={'tp': sides[d]}, device_id_type=MESH)

    def x_copies(a):
        return [pltpu.make_async_copy(
            all_ref.at[pl.ds(pl.multiple_of(shard_of(me, d, a, n) * shard + d * half, 16), half), :],
            x_buf.at[a % 2, pl.ds(d * half, half), :], x_sem.at[a % 2, d]) for d in range(2)]

    def u_copies(a):
        return [pltpu.make_async_copy(
            u_buf.at[a % 2, pl.ds(d * half, half), :],
            u_ref.at[pl.ds(pl.multiple_of(shard_of(me, d, a, n) * shard + d * half, 16), half), :], u_sem.at[a % 2, d]) for d in range(2)]

    load_own = pltpu.make_async_copy(b_ref, x_buf.at[0], x_sem.at[0, 0])
    load_own.start()

    def load_w(t, _):
        for c in w_copies(t):
            c.start()
        return 0

    lax.fori_loop(0, tiles, load_w, 0)
    ring_barrier(right, left)
    for j in range(pieces):
        for d in range(2):
            hop(0, d, j).start()
    load_own.wait()
    keep_own = pltpu.make_async_copy(x_buf.at[0], all_ref.at[pl.ds(pl.multiple_of(me * shard, 16), shard), :], own_sem)
    keep_own.start()
    for a in range(n):
        if a > 0:
            for j in range(pieces):
                for d in range(2):
                    arrival(a - 1, d, j).wait_recv()
                    if a + 1 < n:
                        hop(a, d, j).start()
            if a == 2:
                keep_own.wait()
            for c in x_copies(a):
                c.start()
            for c in x_copies(a):
                c.wait()
        if a >= 2:
            for c in u_copies(a - 2):
                c.wait()

        def one_tile(t, _, a=a):
            if a == 0:
                for c in w_copies(t):
                    c.wait()
            at = pl.multiple_of(t * tile, tile)
            u_buf[a % 2, :, pl.ds(at, tile)] = gated(x_buf[a % 2], w_buf[:, pl.ds(at, tile)], w_buf[:, pl.ds(ff + at, tile)])
            return 0

        lax.fori_loop(0, tiles, one_tile, 0)
        for c in u_copies(a):
            c.start()
    for a in range(max(0, n - 2), n):
        for c in u_copies(a):
            c.wait()
    for a in range(n - 1):
        for j in range(pieces):
            for d in range(2):
                hop(a, d, j).wait_send()


def gather_gate(n, b, w):
    shard, depth = b.shape
    ff = w.shape[1] // 2
    tiles = ff // min(256, ff)
    pieces = 3
    rows = shard * n
    return pl.pallas_call(
        functools.partial(gather_gate_kernel, n, pieces),
        in_specs=[ANY, ANY],
        out_specs=[ANY, ANY],
        out_shape=[jax.ShapeDtypeStruct((rows, depth), BF16), jax.ShapeDtypeStruct((rows, ff), BF16)],
        scratch_shapes=[
            pltpu.VMEM((depth, 2 * ff), BF16),
            pltpu.VMEM((2, shard, depth), BF16),
            pltpu.VMEM((2, shard, ff), BF16),
            pltpu.SemaphoreType.DMA((tiles, 2)),
            pltpu.SemaphoreType.DMA((2, 2)),
            pltpu.SemaphoreType.DMA,
            pltpu.SemaphoreType.DMA((2, 2)),
            pltpu.SemaphoreType.DMA((n - 1, 2, pieces)),
            pltpu.SemaphoreType.DMA((n - 1, 2, pieces)),
        ],
        compiler_params=pltpu.CompilerParams(collective_id=1, has_side_effects=True, vmem_limit_bytes=VMEM_LIMIT),
        cost_estimate=cost(4 * rows * depth * ff * 2, 2 * rows * depth + 2 * w.size),
    )(b, w)


def gate_kernel(x_ref, g_ref, u_ref, o_ref):
    o_ref[...] = gated(x_ref[...], g_ref[...], u_ref[...])


def gate_up(x, w, tile_rows):
    rows, depth = x.shape
    ff = w.shape[1] // 2
    tile = min(256, ff)
    return pl.pallas_call(
        gate_kernel,
        grid=(rows // tile_rows, ff // tile),
        in_specs=[
            pl.BlockSpec((tile_rows, depth), lambda i, j: (i, 0)),
            pl.BlockSpec((depth, tile), lambda i, j: (0, j)),
            pl.BlockSpec((depth, tile), lambda i, j: (0, ff // tile + j)),
        ],
        out_specs=pl.BlockSpec((tile_rows, tile), lambda i, j: (i, j)),
        out_shape=jax.ShapeDtypeStruct((rows, ff), BF16),
        compiler_params=pltpu.CompilerParams(vmem_limit_bytes=VMEM_LIMIT),
        cost_estimate=cost(4 * rows * depth * ff, 2 * rows * depth + 2 * w.size),
    )(x, w, w)


def down_kernel(n, ua_ref, ub_ref, w_ref, r_ref, y_ref, res_buf, res_sem, own_sem, ag_send, ag_recv,
                u_buf, w_buf, s_buf, r_buf, u_sem, w_sem, send_sem, recv_sem):
    me, right, left = ring_place(n)
    sides = (right, left)
    shard = r_ref.shape[0]
    half = shard // 2
    block = w_buf.shape[2]
    blocks = w_ref.shape[1] // block
    load_r = pltpu.make_async_copy(r_ref, res_buf, res_sem)
    load_r.start()
    ring_barrier(right, left)
    load_r.wait()

    def place(d, back, cb):
        row = pl.multiple_of(shard_of(me, d, back, n) * shard + d * half, 16)
        return y_ref.at[pl.ds(row, half), pl.ds(pl.multiple_of(cb * block, block), block)]

    def hop(a, d, cb):
        src = r_buf.at[n - 2, d, cb] if a == 0 else place(d, a, cb)
        return pltpu.make_async_remote_copy(
            src_ref=src, dst_ref=place(d, a, cb), send_sem=ag_send.at[a, d, cb], recv_sem=ag_recv.at[a, d, cb],
            device_id={'tp': sides[d]}, device_id_type=MESH)

    def arrival(a, d, cb):
        return pltpu.make_async_remote_copy(
            src_ref=place(d, a + 1, cb), dst_ref=place(d, a + 1, cb), send_sem=ag_send.at[a, d, cb], recv_sem=ag_recv.at[a, d, cb],
            device_id={'tp': sides[d]}, device_id_type=MESH)

    def keep(d, cb):
        return pltpu.make_async_copy(r_buf.at[n - 2, d, cb], place(d, 0, cb), own_sem.at[d, cb])

    def finish(d, cb, part):
        rows, cols = pl.ds(d * half, half), pl.ds(pl.multiple_of(cb * block, block), block)
        total = res_buf[rows, cols].astype(F32) + part.astype(BF16).astype(F32)
        r_buf[n - 2, d, cb] = total.astype(BF16)
        hop(0, d, cb).start()
        keep(d, cb).start()

    ring_matmul_scatter(n, me, sides, [ua_ref, ub_ref], w_ref, u_buf, w_buf, s_buf, r_buf, u_sem, w_sem, send_sem, recv_sem, finish)
    for a in range(n - 1):
        def forward(cb, _, a=a):
            for d in range(2):
                arrival(a, d, cb).wait_recv()
                if a + 1 < n - 1:
                    hop(a + 1, d, cb).start()
            return 0

        lax.fori_loop(0, blocks, forward, 0)

    def drain(cb, _):
        for d in range(2):
            keep(d, cb).wait()
            for a in range(n - 1):
                hop(a, d, cb).wait_send()
        return 0

    lax.fori_loop(0, blocks, drain, 0)


def down_project(n, act_a, act_b, w_down, resid):
    rows = act_a.shape[0]
    depth, width = w_down.shape
    shard = rows // n
    block = min(512, width // 2)
    blocks = width // block
    return pl.pallas_call(
        functools.partial(down_kernel, n),
        in_specs=[ANY, ANY, ANY, ANY],
        out_specs=ANY,
        out_shape=jax.ShapeDtypeStruct((rows, width), BF16),
        scratch_shapes=[
            pltpu.VMEM((shard, width), BF16), pltpu.SemaphoreType.DMA, pltpu.SemaphoreType.DMA((2, blocks)),
            pltpu.SemaphoreType.DMA((n - 1, 2, blocks)), pltpu.SemaphoreType.DMA((n - 1, 2, blocks)),
        ] + ring_scratch(n, shard // 2, depth, block, blocks, 2),
        compiler_params=pltpu.CompilerParams(collective_id=2, has_side_effects=True, vmem_limit_bytes=VMEM_LIMIT),
        cost_estimate=cost(2 * rows * depth * width * 4, 2 * (rows * depth + depth * width)),
    )(act_a, act_b, w_down, resid)


def gather(shard, axis):
    return lax.all_gather(shard, GROUP_AXES, axis=axis, tiled=True)


def solution(mesh):
    n_tp = mesh.shape['tp']
    assert mesh.shape['cp'] == 2
    seq_spec = P(('dp', 'fsdp'), 'cp', None)
    pos_spec = P(('dp', 'fsdp'), 'cp')
    in_spec = P(GROUP_AXES, 'tp', None)
    out_spec = P('tp', None, GROUP_AXES)
    col_spec = P(GROUP_AXES, 'tp')
    row_spec = P('tp', GROUP_AXES)
    rep_spec = P(None)

    def layer_local(hidden, positions, attn_gain, w_query, w_key, w_value, w_out, mlp_gain, w_gate, w_up, w_down):
        n_seqs, tokens, d_model = hidden.shape
        heads, head = w_query.shape[1:]
        kv_heads = w_key.shape[1]
        rows = n_seqs * tokens
        local = w_query.shape[0]
        ff_half = w_gate.shape[1] // 2
        x = hidden.reshape(rows, d_model)

        w_qkv = jnp.concatenate([w.reshape(local, -1) for w in (w_query, w_key, w_value)], axis=1)
        full_qkv = gather(w_qkv, 0)
        full_out = gather(w_out.reshape(heads * head, -1), 1)
        full_a = gather(jnp.concatenate([w_gate[:, :ff_half], w_up[:, :ff_half]], axis=1), 0)
        full_b = gather(jnp.concatenate([w_gate[:, ff_half:], w_up[:, ff_half:]], axis=1), 0)
        full_down = gather(w_down, 1)

        normed = rms_norm(x.astype(F32), attn_gain)
        inv_freq = ROPE_THETA ** (-jnp.arange(0, head, 2, dtype=F32) / head)
        angles = positions.reshape(rows, 1).astype(F32) * inv_freq
        cos, sin = jnp.cos(angles), jnp.sin(angles)
        cos = jnp.concatenate([cos, cos], axis=1)
        sin = jnp.concatenate([-sin, sin], axis=1)

        q_width, kv_width = heads * head, 2 * kv_heads * head
        kv = project(normed, full_qkv, cos, sin, q_width // kv_width, kv_width, kv_heads, head)
        kv_peer = lax.ppermute(kv, 'cp', [(0, 1), (1, 0)])
        q = project(normed, full_qkv, cos, sin, 0, q_width, heads, head)
        mixed = attention(q, kv, kv_peer, n_seqs, kv_heads, heads // kv_heads, head)
        resid, normed_mlp = out_project(n_tp, mixed, full_out, x, mlp_gain.reshape(1, d_model))
        all_normed, act_a = gather_gate(n_tp, normed_mlp, full_a)
        act_b = gate_up(all_normed, full_b, rows // n_tp)
        y = down_project(n_tp, act_a, act_b, full_down, resid)
        return y.reshape(hidden.shape)

    return jax.shard_map(
        layer_local, mesh=mesh,
        in_specs=(seq_spec, pos_spec, rep_spec, in_spec, in_spec, in_spec, out_spec, rep_spec, col_spec, col_spec, row_spec),
        out_specs=seq_spec, check_vma=False)
```

```python
import functools
import math

import jax
import jax.numpy as jnp
from jax import lax
from jax.experimental import pallas as pl
from jax.experimental.pallas import tpu as pltpu
from jax.sharding import PartitionSpec as P


ROPE_THETA = 500000.0
NORM_EPS = 1e-5
GROUP_AXES = ('fsdp', 'cp')
VMEM_LIMIT = 62 * 1024 * 1024
F32 = jnp.float32
BF16 = jnp.bfloat16
MESH = pl.DeviceIdType.MESH
ANY = pl.BlockSpec(memory_space=pl.ANY)
VMEM = pl.BlockSpec(memory_space=pltpu.VMEM)


def rms_norm(hidden_f32, gain):
    mean_sq = jnp.mean(hidden_f32 * hidden_f32, axis=-1, keepdims=True)
    return (hidden_f32 * lax.rsqrt(mean_sq + NORM_EPS) * gain).astype(BF16)


def cost(flops, bytes_accessed):
    return pl.CostEstimate(flops=int(flops), bytes_accessed=int(bytes_accessed), transcendentals=0)


def proj_kernel(rope_heads, head, x_ref, w_ref, cos_ref, sin_ref, o_ref):
    acc = jnp.dot(x_ref[...], w_ref[...], preferred_element_type=F32)
    cos, sin = cos_ref[...], sin_ref[...]
    for i in range(acc.shape[1] // head):
        part = acc[:, i * head:(i + 1) * head]
        if i < rope_heads:
            part = part * cos + pltpu.roll(part, head // 2, 1) * sin
        o_ref[:, i * head:(i + 1) * head] = part.astype(BF16)


def project(x, w, cos, sin, col_block, width, rope_heads, head, tile=256):
    rows, depth = x.shape
    tile = math.gcd(tile, rows)
    return pl.pallas_call(
        functools.partial(proj_kernel, rope_heads, head),
        grid=(rows // tile,),
        in_specs=[
            pl.BlockSpec((tile, depth), lambda i: (i, 0)),
            pl.BlockSpec((depth, width), lambda i: (0, col_block)),
            pl.BlockSpec((tile, head), lambda i: (i, 0)),
            pl.BlockSpec((tile, head), lambda i: (i, 0)),
        ],
        out_specs=pl.BlockSpec((tile, width), lambda i: (i, 0)),
        out_shape=jax.ShapeDtypeStruct((rows, width), BF16),
        compiler_params=pltpu.CompilerParams(vmem_limit_bytes=VMEM_LIMIT),
        cost_estimate=cost(2 * rows * depth * width, 2 * (rows * depth + depth * width + rows * width)),
    )(x, w, cos, sin)


def attn_kernel(group, head, seg, q_ref, ko_ref, vo_ref, kp_ref, vp_ref, o_ref):
    c = lax.axis_index('cp')
    scale = head ** -0.5 * math.log2(math.e)

    def run(first_full, second_full):
        low, high = pl.ds(0, seg), pl.ds(seg, seg)
        own_low, own_high = (ko_ref, vo_ref, low), (ko_ref, vo_ref, high)
        tri = lax.broadcasted_iota(jnp.int32, (seg, seg), 0) >= lax.broadcasted_iota(jnp.int32, (seg, seg), 1)
        for g in range(group):
            cols = pl.ds(g * head, head)
            for rows, diag, full in ((low, own_low, first_full), (high, own_high, second_full)):
                q = q_ref[rows, cols]
                blocks = full + [diag]
                scores = []
                for k_ref, _, part in blocks:
                    scores.append(lax.dot_general(q, k_ref[part, :], (((1,), (1,)), ((), ())), preferred_element_type=F32))
                scores[-1] = jnp.where(tri, scores[-1], -jnp.inf)
                top = functools.reduce(jnp.maximum, [jnp.max(s, axis=-1, keepdims=True) for s in scores])
                total = jnp.zeros((seg, 1), F32)
                out = jnp.zeros((seg, head), F32)
                for s, (_, v_ref, part) in zip(scores, blocks):
                    p = jnp.exp2((s - top) * scale)
                    total = total + jnp.sum(p, axis=-1, keepdims=True)
                    out = out + jnp.dot(p.astype(BF16), v_ref[part, :], preferred_element_type=F32)
                o_ref[rows, cols] = (out / total).astype(BF16)

    low, high = pl.ds(0, seg), pl.ds(seg, seg)
    own_low, peer_low, peer_high = (ko_ref, vo_ref, low), (kp_ref, vp_ref, low), (kp_ref, vp_ref, high)

    @pl.when(c == 0)
    def _():
        run([], [own_low, peer_low, peer_high])

    @pl.when(c == 1)
    def _():
        run([peer_low], [peer_low, own_low])


def attention(q, kv_own, kv_peer, n_seqs, kv_heads, group, head):
    rows = q.shape[0]
    tokens = rows // n_seqs
    q_spec = pl.BlockSpec((tokens, group * head), lambda i, h: (i, h))
    k_spec = pl.BlockSpec((tokens, head), lambda i, h: (i, h))
    v_spec = pl.BlockSpec((tokens, head), lambda i, h: (i, kv_heads + h))
    return pl.pallas_call(
        functools.partial(attn_kernel, group, head, tokens // 2),
        grid=(n_seqs, kv_heads),
        in_specs=[q_spec, k_spec, v_spec, k_spec, v_spec],
        out_specs=q_spec,
        out_shape=jax.ShapeDtypeStruct(q.shape, BF16),
        compiler_params=pltpu.CompilerParams(vmem_limit_bytes=VMEM_LIMIT),
        cost_estimate=cost(10 * rows * tokens * kv_heads * group * head, 4 * q.size),
    )(q, kv_own, kv_own, kv_peer, kv_peer)


def ring_barrier(right, left):
    barrier = pltpu.get_barrier_semaphore()
    for neighbour in (right, left):
        pl.semaphore_signal(barrier, inc=1, device_id={'tp': neighbour}, device_id_type=MESH)
    pl.semaphore_wait(barrier, 2)


def ring_place(n):
    me = lax.axis_index('tp')
    return me, lax.rem(me + 1, n), lax.rem(me + n - 1, n)


def shard_of(me, direction, back, n):
    return lax.rem(me + (n - back if direction == 0 else back), n)


def ring_matmul_scatter(n, me, sides, u_refs, w_ref, u_buf, w_buf, s_buf, r_buf, u_sem, w_sem, send_sem, recv_sem, finish, hook=None):
    half = u_buf.shape[2]
    block = w_buf.shape[2]
    blocks = w_ref.shape[1] // block

    def u_copies(step):
        copies = []
        for d in range(2):
            row = pl.multiple_of(shard_of(me, d, step + 1, n) * (2 * half) + d * half, 16)
            at = 0
            for i, u_ref in enumerate(u_refs):
                copies.append(pltpu.make_async_copy(
                    u_ref.at[pl.ds(row, half), :], u_buf.at[step % 2, d, :, pl.ds(at, u_ref.shape[1])], u_sem.at[step % 2, d, i]))
                at += u_ref.shape[1]
        return copies

    def w_copy(cb, slot):
        return pltpu.make_async_copy(w_ref.at[:, pl.ds(pl.multiple_of(cb * block, block), block)], w_buf.at[slot], w_sem.at[slot])

    def send(step, d, cb):
        src = s_buf.at[d, cb] if step == 0 else r_buf.at[step - 1, d, cb]
        return pltpu.make_async_remote_copy(
            src_ref=src, dst_ref=r_buf.at[step, d, cb], send_sem=send_sem.at[step, d, cb], recv_sem=recv_sem.at[step, d, cb],
            device_id={'tp': sides[d]}, device_id_type=MESH)

    for c in u_copies(0):
        c.start()
    w_copy(0, 0).start()
    for step in range(n):
        for c in u_copies(step):
            c.wait()
        if step + 1 < n:
            for c in u_copies(step + 1):
                c.start()

        def one_block(cb, _, step=step):
            slot = lax.rem(cb, 2)
            w_copy(cb, slot).wait()
            if step + 1 < n:
                w_copy(lax.rem(cb + 1, blocks), 1 - slot).start()
            else:
                @pl.when(cb + 1 < blocks)
                def _():
                    w_copy(cb + 1, 1 - slot).start()
            parts = [jnp.dot(u_buf[step % 2, d], w_buf[slot], preferred_element_type=F32) for d in range(2)]
            for d in range(2):
                part = parts[d]
                if step > 0:
                    send(step - 1, d, cb).wait_recv()
                    part = part + r_buf[step - 1, d, cb].astype(F32)
                if step + 1 < n:
                    if step == 0:
                        s_buf[d, cb] = part.astype(BF16)
                    else:
                        r_buf[step - 1, d, cb] = part.astype(BF16)
                    send(step, d, cb).start()
                else:
                    finish(d, cb, part)
            if hook is not None:
                hook(step, cb)
            return 0

        lax.fori_loop(0, blocks, one_block, 0)

    def drain(cb, _):
        for step in range(n - 1):
            for d in range(2):
                send(step, d, cb).wait_send()
        return 0

    lax.fori_loop(0, blocks, drain, 0)


def ring_scratch(n, half, depth, block, blocks, n_u):
    return [
        pltpu.VMEM((2, 2, half, depth), BF16),
        pltpu.VMEM((2, depth, block), BF16),
        pltpu.VMEM((2, blocks, half, block), BF16),
        pltpu.VMEM((n - 1, 2, blocks, half, block), BF16),
        pltpu.SemaphoreType.DMA((2, 2, n_u)),
        pltpu.SemaphoreType.DMA((2,)),
        pltpu.SemaphoreType.DMA((n - 1, 2, blocks)),
        pltpu.SemaphoreType.DMA((n - 1, 2, blocks)),
    ]


def out_kernel(n, o_ref, w_ref, h_ref, gain_ref, r_ref, b_ref, h_buf, h_sem, u_buf, w_buf, s_buf, r_buf, u_sem, w_sem, send_sem, recv_sem):
    me, right, left = ring_place(n)
    shard, _ = r_ref.shape
    half = shard // 2
    block = w_buf.shape[2]
    load_h = pltpu.make_async_copy(h_ref.at[pl.ds(pl.multiple_of(me * shard, 16), shard), :], h_buf, h_sem)
    load_h.start()
    ring_barrier(right, left)
    load_h.wait()

    def finish(d, cb, part):
        rows, cols = pl.ds(d * half, half), pl.ds(pl.multiple_of(cb * block, block), block)
        total = h_buf[rows, cols].astype(F32) + part.astype(BF16).astype(F32)
        r_ref[rows, cols] = total.astype(BF16)

    ring_matmul_scatter(n, me, (right, left), [o_ref], w_ref, u_buf, w_buf, s_buf, r_buf, u_sem, w_sem, send_sem, recv_sem, finish)
    gain = gain_ref[...]

    def norm_rows(i, _):
        rows = pl.ds(pl.multiple_of(i * 16, 16), 16)
        b_ref[rows, :] = rms_norm(r_ref[rows, :].astype(F32), gain)
        return 0

    lax.fori_loop(0, shard // 16, norm_rows, 0)


def out_project(n, mixed, w_out, hidden, gain):
    rows, depth = mixed.shape
    width = w_out.shape[1]
    shard = rows // n
    block = min(512, width // 2)
    blocks = width // block
    return pl.pallas_call(
        functools.partial(out_kernel, n),
        in_specs=[ANY, ANY, ANY, VMEM],
        out_specs=[VMEM, VMEM],
        out_shape=[jax.ShapeDtypeStruct((shard, width), BF16)] * 2,
        scratch_shapes=[pltpu.VMEM((shard, width), BF16), pltpu.SemaphoreType.DMA]
        + ring_scratch(n, shard // 2, depth, block, blocks, 1),
        compiler_params=pltpu.CompilerParams(collective_id=0, has_side_effects=True, vmem_limit_bytes=VMEM_LIMIT),
        cost_estimate=cost(2 * rows * depth * width * 5, 2 * (rows * depth + depth * width)),
    )(mixed, w_out, hidden, gain)


def gated(x, w_gate, w_up):
    gate = jnp.dot(x, w_gate, preferred_element_type=F32)
    up = jnp.dot(x, w_up, preferred_element_type=F32)
    return (jax.nn.silu(gate) * up).astype(BF16)


def gather_gate_kernel(n, pieces, b_ref, w_ref, all_ref, u_ref, w_buf, x_buf, u_buf, w_sem, x_sem, own_sem, u_sem, send_sem, recv_sem):
    me, right, left = ring_place(n)
    sides = (right, left)
    shard = b_ref.shape[0]
    half = shard // 2
    piece = half // pieces
    ff = u_ref.shape[1]
    tile = min(256, ff)
    tiles = ff // tile
    turns = [(a, j) for a in range(n) for j in range(pieces)]

    def w_copies(t):
        out = []
        for i in range(2):
            cols = pl.ds(pl.multiple_of(i * ff + t * tile, tile), tile)
            out.append(pltpu.make_async_copy(w_ref.at[:, cols], w_buf.at[:, cols], w_sem.at[t, i]))
        return out

    def rows_of(d, back, j):
        return pl.ds(pl.multiple_of(shard_of(me, d, back, n) * shard + d * half + j * piece, 16), piece)

    def own_rows(d, j):
        return b_ref.at[pl.ds(d * half + j * piece, piece), :]

    def hop(a, d, j):
        rows = rows_of(d, a, j)
        return pltpu.make_async_remote_copy(
            src_ref=own_rows(d, j) if a == 0 else all_ref.at[rows, :], dst_ref=all_ref.at[rows, :],
            send_sem=send_sem.at[a, d, j], recv_sem=recv_sem.at[a, d, j], device_id={'tp': sides[d]}, device_id_type=MESH)

    def arrival(a, d, j):
        rows = rows_of(d, a + 1, j)
        return pltpu.make_async_remote_copy(
            src_ref=all_ref.at[rows, :], dst_ref=all_ref.at[rows, :], send_sem=send_sem.at[a, d, j], recv_sem=recv_sem.at[a, d, j],
            device_id={'tp': sides[d]}, device_id_type=MESH)

    def x_copies(k):
        a, j = turns[k]
        return [pltpu.make_async_copy(
            own_rows(d, j) if a == 0 else all_ref.at[rows_of(d, a, j), :],
            x_buf.at[k % 2, pl.ds(d * piece, piece), :], x_sem.at[k % 2, d]) for d in range(2)]

    def keep_copies(k):
        a, j = turns[k]
        return [pltpu.make_async_copy(
            x_buf.at[k % 2, pl.ds(d * piece, piece), :], all_ref.at[rows_of(d, a, j), :], own_sem.at[j, d]) for d in range(2)]

    def u_copies(k):
        a, j = turns[k]
        return [pltpu.make_async_copy(
            u_buf.at[k % 2, pl.ds(d * piece, piece), :], u_ref.at[rows_of(d, a, j), :], u_sem.at[k % 2, d]) for d in range(2)]

    def start(copies):
        for c in copies:
            c.start()

    def wait(copies):
        for c in copies:
            c.wait()

    start(x_copies(0))

    def load_w(t, _):
        start(w_copies(t))
        return 0

    lax.fori_loop(0, tiles, load_w, 0)
    ring_barrier(right, left)
    for j in range(pieces):
        for d in range(2):
            hop(0, d, j).start()
    for k, (a, j) in enumerate(turns):
        if a > 0:
            for d in range(2):
                arrival(a - 1, d, j).wait_recv()
                if a + 1 < n:
                    hop(a, d, j).start()
            start(x_copies(k))
        wait(x_copies(k))
        if a == 0:
            start(keep_copies(k))
            if j > 0:
                wait(keep_copies(k - 1))
            if j + 1 < pieces:
                start(x_copies(k + 1))
        elif j == 0 and a == 1:
            wait(keep_copies(k - 1))
        if k >= 2:
            wait(u_copies(k - 2))

        def one_tile(t, _, k=k):
            if k == 0:
                wait(w_copies(t))
            at = pl.multiple_of(t * tile, tile)
            u_buf[k % 2, :, pl.ds(at, tile)] = gated(x_buf[k % 2], w_buf[:, pl.ds(at, tile)], w_buf[:, pl.ds(ff + at, tile)])
            return 0

        lax.fori_loop(0, tiles, one_tile, 0)
        start(u_copies(k))
    for k in range(len(turns) - 2, len(turns)):
        wait(u_copies(k))
    for a in range(n - 1):
        for j in range(pieces):
            for d in range(2):
                hop(a, d, j).wait_send()


def gather_gate(n, b, w):
    shard, depth = b.shape
    ff = w.shape[1] // 2
    tiles = ff // min(256, ff)
    pieces = 3
    piece = shard // 2 // pieces
    rows = shard * n
    return pl.pallas_call(
        functools.partial(gather_gate_kernel, n, pieces),
        in_specs=[ANY, ANY],
        out_specs=[ANY, ANY],
        out_shape=[jax.ShapeDtypeStruct((rows, depth), BF16), jax.ShapeDtypeStruct((rows, ff), BF16)],
        scratch_shapes=[
            pltpu.VMEM((depth, 2 * ff), BF16),
            pltpu.VMEM((2, 2 * piece, depth), BF16),
            pltpu.VMEM((2, 2 * piece, ff), BF16),
            pltpu.SemaphoreType.DMA((tiles, 2)),
            pltpu.SemaphoreType.DMA((2, 2)),
            pltpu.SemaphoreType.DMA((pieces, 2)),
            pltpu.SemaphoreType.DMA((2, 2)),
            pltpu.SemaphoreType.DMA((n - 1, 2, pieces)),
            pltpu.SemaphoreType.DMA((n - 1, 2, pieces)),
        ],
        compiler_params=pltpu.CompilerParams(collective_id=1, has_side_effects=True, vmem_limit_bytes=VMEM_LIMIT),
        cost_estimate=cost(4 * rows * depth * ff * 2, 2 * rows * depth + 2 * w.size),
    )(b, w)


def gate_kernel(x_ref, g_ref, u_ref, o_ref):
    o_ref[...] = gated(x_ref[...], g_ref[...], u_ref[...])


def gate_up(x, w, tile_rows):
    rows, depth = x.shape
    ff = w.shape[1] // 2
    tile = min(256, ff)
    return pl.pallas_call(
        gate_kernel,
        grid=(rows // tile_rows, ff // tile),
        in_specs=[
            pl.BlockSpec((tile_rows, depth), lambda i, j: (i, 0)),
            pl.BlockSpec((depth, tile), lambda i, j: (0, j)),
            pl.BlockSpec((depth, tile), lambda i, j: (0, ff // tile + j)),
        ],
        out_specs=pl.BlockSpec((tile_rows, tile), lambda i, j: (i, j)),
        out_shape=jax.ShapeDtypeStruct((rows, ff), BF16),
        compiler_params=pltpu.CompilerParams(vmem_limit_bytes=VMEM_LIMIT),
        cost_estimate=cost(4 * rows * depth * ff, 2 * rows * depth + 2 * w.size),
    )(x, w, w)


def part_cols(part, block, cb):
    return pl.ds(pl.multiple_of((2 * cb + part) * block, block), block)


def load_resid(r_ref, res_buf, res_sem, part, block, blocks):
    def copy(cb):
        return pltpu.make_async_copy(r_ref.at[:, part_cols(part, block, cb)], res_buf.at[cb], res_sem.at[cb])

    def begin(cb, _):
        copy(cb).start()
        return 0

    def end(cb, _):
        copy(cb).wait()
        return 0

    return lambda: lax.fori_loop(0, blocks, begin, 0), lambda: lax.fori_loop(0, blocks, end, 0)


def down_sum_kernel(n, ua_ref, ub_ref, w_ref, r_ref, y_ref, res_buf, res_sem, u_buf, w_buf, s_buf, r_buf, u_sem, w_sem, send_sem, recv_sem):
    me, right, left = ring_place(n)
    half = r_ref.shape[0] // 2
    blocks, _, block = res_buf.shape
    begin, end = load_resid(r_ref, res_buf, res_sem, 0, block, blocks)
    begin()
    ring_barrier(right, left)
    end()

    def finish(d, cb, part):
        total = res_buf[cb, pl.ds(d * half, half), :].astype(F32) + part.astype(BF16).astype(F32)
        y_ref[d, cb] = total.astype(BF16)

    ring_matmul_scatter(n, me, (right, left), [ua_ref, ub_ref], w_ref, u_buf, w_buf, s_buf, r_buf, u_sem, w_sem, send_sem, recv_sem, finish)


def down_kernel(n, ua_ref, ub_ref, w_ref, r_ref, first_ref, y_ref, res_buf, res_sem, own_sem, ag_send, ag_recv,
                u_buf, w_buf, s_buf, r_buf, u_sem, w_sem, send_sem, recv_sem):
    me, right, left = ring_place(n)
    sides = (right, left)
    shard = r_ref.shape[0]
    half = shard // 2
    blocks, _, block = res_buf.shape
    begin, end = load_resid(r_ref, res_buf, res_sem, 1, block, blocks)
    begin()
    ring_barrier(right, left)

    def place(d, back, part, cb):
        row = pl.multiple_of(shard_of(me, d, back, n) * shard + d * half, 16)
        return y_ref.at[pl.ds(row, half), part_cols(part, block, cb)]

    def own(d, part, cb):
        return first_ref.at[d, cb] if part == 0 else r_buf.at[n - 2, d, cb]

    def hop(a, d, part, cb):
        return pltpu.make_async_remote_copy(
            src_ref=own(d, part, cb) if a == 0 else place(d, a, part, cb), dst_ref=place(d, a, part, cb),
            send_sem=ag_send.at[a, d, part, cb], recv_sem=ag_recv.at[a, d, part, cb], device_id={'tp': sides[d]}, device_id_type=MESH)

    def arrival(a, d, part, cb):
        return pltpu.make_async_remote_copy(
            src_ref=place(d, a + 1, part, cb), dst_ref=place(d, a + 1, part, cb),
            send_sem=ag_send.at[a, d, part, cb], recv_sem=ag_recv.at[a, d, part, cb], device_id={'tp': sides[d]}, device_id_type=MESH)

    def keep(d, part, cb):
        return pltpu.make_async_copy(own(d, part, cb), place(d, 0, part, cb), own_sem.at[d, part, cb])

    def forward(a, part, cb):
        for d in range(2):
            arrival(a, d, part, cb).wait_recv()
            if a + 1 < n - 1:
                hop(a + 1, d, part, cb).start()

    def send_first(cb, _):
        for d in range(2):
            hop(0, d, 0, cb).start()
            keep(d, 0, cb).start()
        return 0

    lax.fori_loop(0, blocks, send_first, 0)
    end()

    def finish(d, cb, part):
        total = res_buf[cb, pl.ds(d * half, half), :].astype(F32) + part.astype(BF16).astype(F32)
        r_buf[n - 2, d, cb] = total.astype(BF16)
        hop(0, d, 1, cb).start()
        keep(d, 1, cb).start()

    def hook(step, cb):
        if step > 0:
            forward(step - 1, 0, cb)

    ring_matmul_scatter(n, me, sides, [ua_ref, ub_ref], w_ref, u_buf, w_buf, s_buf, r_buf, u_sem, w_sem, send_sem, recv_sem, finish, hook)
    for a in range(n - 1):
        def last(cb, _, a=a):
            forward(a, 1, cb)
            return 0

        lax.fori_loop(0, blocks, last, 0)

    def drain(cb, _):
        for part in range(2):
            for d in range(2):
                keep(d, part, cb).wait()
                for a in range(n - 1):
                    hop(a, d, part, cb).wait_send()
        return 0

    lax.fori_loop(0, blocks, drain, 0)


def down_project(n, act_a, act_b, w_first, w_second, resid, blocks):
    rows = act_a.shape[0]
    depth, part = w_first.shape
    shard = rows // n
    block = part // blocks
    half = shard // 2
    resid_scratch = [pltpu.VMEM((blocks, shard, block), BF16), pltpu.SemaphoreType.DMA((blocks,))]
    ring = ring_scratch(n, half, depth, block, blocks, 2)
    params = dict(has_side_effects=True, vmem_limit_bytes=VMEM_LIMIT)
    first = pl.pallas_call(
        functools.partial(down_sum_kernel, n),
        in_specs=[ANY] * 4,
        out_specs=VMEM,
        out_shape=jax.ShapeDtypeStruct((2, blocks, half, block), BF16),
        scratch_shapes=resid_scratch + ring,
        compiler_params=pltpu.CompilerParams(collective_id=2, **params),
        cost_estimate=cost(2 * rows * depth * part * 2, 2 * (rows * depth + depth * part)),
    )(act_a, act_b, w_first, resid)
    return pl.pallas_call(
        functools.partial(down_kernel, n),
        in_specs=[ANY] * 5,
        out_specs=ANY,
        out_shape=jax.ShapeDtypeStruct((rows, 2 * part), BF16),
        scratch_shapes=resid_scratch + [
            pltpu.SemaphoreType.DMA((2, 2, blocks)),
            pltpu.SemaphoreType.DMA((n - 1, 2, 2, blocks)), pltpu.SemaphoreType.DMA((n - 1, 2, 2, blocks)),
        ] + ring,
        compiler_params=pltpu.CompilerParams(collective_id=3, **params),
        cost_estimate=cost(2 * rows * depth * part * 6, 2 * (rows * depth + depth * part)),
    )(act_a, act_b, w_second, resid, first)


def gather(shard, axis):
    return lax.all_gather(shard, GROUP_AXES, axis=axis, tiled=True)


def solution(mesh):
    n_tp = mesh.shape['tp']
    assert mesh.shape['cp'] == 2
    seq_spec = P(('dp', 'fsdp'), 'cp', None)
    pos_spec = P(('dp', 'fsdp'), 'cp')
    in_spec = P(GROUP_AXES, 'tp', None)
    out_spec = P('tp', None, GROUP_AXES)
    col_spec = P(GROUP_AXES, 'tp')
    row_spec = P('tp', GROUP_AXES)
    rep_spec = P(None)

    def layer_local(hidden, positions, attn_gain, w_query, w_key, w_value, w_out, mlp_gain, w_gate, w_up, w_down):
        n_seqs, tokens, d_model = hidden.shape
        heads, head = w_query.shape[1:]
        kv_heads = w_key.shape[1]
        rows = n_seqs * tokens
        local = w_query.shape[0]
        ff_a = w_gate.shape[1] * 9 // 14 // 256 * 256
        x = hidden.reshape(rows, d_model)

        w_qkv = jnp.concatenate([w.reshape(local, -1) for w in (w_query, w_key, w_value)], axis=1)
        full_qkv = gather(w_qkv, 0)
        full_out = gather(w_out.reshape(heads * head, -1), 1)
        full_a = gather(jnp.concatenate([w_gate[:, :ff_a], w_up[:, :ff_a]], axis=1), 0)
        full_b = gather(jnp.concatenate([w_gate[:, ff_a:], w_up[:, ff_a:]], axis=1), 0)
        down_half = w_down.shape[1] // 2
        full_down0 = gather(w_down[:, :down_half], 1)
        full_down1 = gather(w_down[:, down_half:], 1)

        normed = rms_norm(x.astype(F32), attn_gain)
        inv_freq = ROPE_THETA ** (-jnp.arange(0, head, 2, dtype=F32) / head)
        angles = positions.reshape(rows, 1).astype(F32) * inv_freq
        cos, sin = jnp.cos(angles), jnp.sin(angles)
        cos = jnp.concatenate([cos, cos], axis=1)
        sin = jnp.concatenate([-sin, sin], axis=1)

        q_width, kv_width = heads * head, 2 * kv_heads * head
        kv = project(normed, full_qkv, cos, sin, q_width // kv_width, kv_width, kv_heads, head)
        kv_peer = lax.ppermute(kv, 'cp', [(0, 1), (1, 0)])
        q = project(normed, full_qkv, cos, sin, 0, q_width, heads, head)
        mixed = attention(q, kv, kv_peer, n_seqs, kv_heads, heads // kv_heads, head)
        resid, normed_mlp = out_project(n_tp, mixed, full_out, x, mlp_gain.reshape(1, d_model))
        all_normed, act_a = gather_gate(n_tp, normed_mlp, full_a)
        act_b = gate_up(all_normed, full_b, rows // n_tp)
        y = down_project(n_tp, act_a, act_b, full_down0, full_down1, resid, full_down0.shape[1] // down_half)
        return y.reshape(hidden.shape)

    return jax.shard_map(
        layer_local, mesh=mesh,
        in_specs=(seq_spec, pos_spec, rep_spec, in_spec, in_spec, in_spec, out_spec, rep_spec, col_spec, col_spec, row_spec),
        out_specs=seq_spec, check_vma=False)
```

```python
import functools
import math

import jax
import jax.numpy as jnp
from jax import lax
from jax.experimental import pallas as pl
from jax.experimental.pallas import tpu as pltpu
from jax.sharding import PartitionSpec as P


ROPE_THETA = 500000.0
NORM_EPS = 1e-5
GROUP_AXES = ('fsdp', 'cp')
VMEM_LIMIT = 62 * 1024 * 1024
F32 = jnp.float32
BF16 = jnp.bfloat16
MESH = pl.DeviceIdType.MESH
ANY = pl.BlockSpec(memory_space=pl.ANY)
VMEM = pl.BlockSpec(memory_space=pltpu.VMEM)


def rms_norm(hidden_f32, gain):
    mean_sq = jnp.mean(hidden_f32 * hidden_f32, axis=-1, keepdims=True)
    return (hidden_f32 * lax.rsqrt(mean_sq + NORM_EPS) * gain).astype(BF16)


def cost(flops, bytes_accessed):
    return pl.CostEstimate(flops=int(flops), bytes_accessed=int(bytes_accessed), transcendentals=0)


def proj_kernel(rope_heads, head, x_ref, w_ref, cos_ref, sin_ref, o_ref):
    acc = jnp.dot(x_ref[...], w_ref[...], preferred_element_type=F32)
    cos, sin = cos_ref[...], sin_ref[...]
    for i in range(acc.shape[1] // head):
        part = acc[:, i * head:(i + 1) * head]
        if i < rope_heads:
            part = part * cos + pltpu.roll(part, head // 2, 1) * sin
        o_ref[:, i * head:(i + 1) * head] = part.astype(BF16)


def project(x, w, cos, sin, col_block, width, rope_heads, head, tile=256):
    rows, depth = x.shape
    tile = math.gcd(tile, rows)
    return pl.pallas_call(
        functools.partial(proj_kernel, rope_heads, head),
        grid=(rows // tile,),
        in_specs=[
            pl.BlockSpec((tile, depth), lambda i: (i, 0)),
            pl.BlockSpec((depth, width), lambda i: (0, col_block)),
            pl.BlockSpec((tile, head), lambda i: (i, 0)),
            pl.BlockSpec((tile, head), lambda i: (i, 0)),
        ],
        out_specs=pl.BlockSpec((tile, width), lambda i: (i, 0)),
        out_shape=jax.ShapeDtypeStruct((rows, width), BF16),
        compiler_params=pltpu.CompilerParams(vmem_limit_bytes=VMEM_LIMIT),
        cost_estimate=cost(2 * rows * depth * width, 2 * (rows * depth + depth * width + rows * width)),
    )(x, w, cos, sin)


def attn_kernel(group, head, seg, q_ref, ko_ref, vo_ref, kp_ref, vp_ref, o_ref):
    c = lax.axis_index('cp')
    scale = head ** -0.5 * math.log2(math.e)

    def run(first_full, second_full):
        low, high = pl.ds(0, seg), pl.ds(seg, seg)
        own_low, own_high = (ko_ref, vo_ref, low), (ko_ref, vo_ref, high)
        tri = lax.broadcasted_iota(jnp.int32, (seg, seg), 0) >= lax.broadcasted_iota(jnp.int32, (seg, seg), 1)
        for g in range(group):
            cols = pl.ds(g * head, head)
            for rows, diag, full in ((low, own_low, first_full), (high, own_high, second_full)):
                q = q_ref[rows, cols]
                blocks = full + [diag]
                scores = []
                for k_ref, _, part in blocks:
                    scores.append(lax.dot_general(q, k_ref[part, :], (((1,), (1,)), ((), ())), preferred_element_type=F32))
                scores[-1] = jnp.where(tri, scores[-1], -jnp.inf)
                top = functools.reduce(jnp.maximum, [jnp.max(s, axis=-1, keepdims=True) for s in scores])
                total = jnp.zeros((seg, 1), F32)
                out = jnp.zeros((seg, head), F32)
                for s, (_, v_ref, part) in zip(scores, blocks):
                    p = jnp.exp2((s - top) * scale)
                    total = total + jnp.sum(p, axis=-1, keepdims=True)
                    out = out + jnp.dot(p.astype(BF16), v_ref[part, :], preferred_element_type=F32)
                o_ref[rows, cols] = (out / total).astype(BF16)

    low, high = pl.ds(0, seg), pl.ds(seg, seg)
    own_low, peer_low, peer_high = (ko_ref, vo_ref, low), (kp_ref, vp_ref, low), (kp_ref, vp_ref, high)

    @pl.when(c == 0)
    def _():
        run([], [own_low, peer_low, peer_high])

    @pl.when(c == 1)
    def _():
        run([peer_low], [peer_low, own_low])


def attention(q, kv_own, kv_peer, n_seqs, kv_heads, group, head):
    rows = q.shape[0]
    tokens = rows // n_seqs
    q_spec = pl.BlockSpec((tokens, group * head), lambda i, h: (i, h))
    k_spec = pl.BlockSpec((tokens, head), lambda i, h: (i, h))
    v_spec = pl.BlockSpec((tokens, head), lambda i, h: (i, kv_heads + h))
    return pl.pallas_call(
        functools.partial(attn_kernel, group, head, tokens // 2),
        grid=(n_seqs, kv_heads),
        in_specs=[q_spec, k_spec, v_spec, k_spec, v_spec],
        out_specs=q_spec,
        out_shape=jax.ShapeDtypeStruct(q.shape, BF16),
        compiler_params=pltpu.CompilerParams(vmem_limit_bytes=VMEM_LIMIT),
        cost_estimate=cost(10 * rows * tokens * kv_heads * group * head, 4 * q.size),
    )(q, kv_own, kv_own, kv_peer, kv_peer)


def ring_barrier(right, left):
    barrier = pltpu.get_barrier_semaphore()
    for neighbour in (right, left):
        pl.semaphore_signal(barrier, inc=1, device_id={'tp': neighbour}, device_id_type=MESH)
    pl.semaphore_wait(barrier, 2)


def ring_place(n):
    me = lax.axis_index('tp')
    return me, lax.rem(me + 1, n), lax.rem(me + n - 1, n)


def shard_of(me, direction, back, n):
    return lax.rem(me + (n - back if direction == 0 else back), n)


def ring_matmul_scatter(n, me, sides, u_refs, w_ref, u_buf, w_buf, s_buf, r_buf, u_sem, w_sem, send_sem, recv_sem, finish, hook=None, prepare=None):
    half = u_buf.shape[2]
    block = w_buf.shape[2]
    blocks = w_ref.shape[1] // block

    def u_copies(step):
        copies = []
        for d in range(2):
            row = pl.multiple_of(shard_of(me, d, step + 1, n) * (2 * half) + d * half, 16)
            at = 0
            for i, u_ref in enumerate(u_refs):
                copies.append(pltpu.make_async_copy(
                    u_ref.at[pl.ds(row, half), :], u_buf.at[step % 2, d, :, pl.ds(at, u_ref.shape[1])], u_sem.at[step % 2, d, i]))
                at += u_ref.shape[1]
        return copies

    def w_copy(cb, slot):
        return pltpu.make_async_copy(w_ref.at[:, pl.ds(pl.multiple_of(cb * block, block), block)], w_buf.at[slot], w_sem.at[slot])

    def send(step, d, cb):
        src = s_buf.at[d, cb] if step == 0 else r_buf.at[step - 1, d, cb]
        return pltpu.make_async_remote_copy(
            src_ref=src, dst_ref=r_buf.at[step, d, cb], send_sem=send_sem.at[step, d, cb], recv_sem=recv_sem.at[step, d, cb],
            device_id={'tp': sides[d]}, device_id_type=MESH)

    for c in u_copies(0):
        c.start()
    w_copy(0, 0).start()
    for step in range(n):
        for c in u_copies(step):
            c.wait()
        if step + 1 < n:
            for c in u_copies(step + 1):
                c.start()
        if prepare is not None:
            prepare(step)

        def one_block(cb, _, step=step):
            slot = lax.rem(cb, 2)
            w_copy(cb, slot).wait()
            if step + 1 < n:
                w_copy(lax.rem(cb + 1, blocks), 1 - slot).start()
            else:
                @pl.when(cb + 1 < blocks)
                def _():
                    w_copy(cb + 1, 1 - slot).start()
            parts = [jnp.dot(u_buf[step % 2, d], w_buf[slot], preferred_element_type=F32) for d in range(2)]
            for d in range(2):
                part = parts[d]
                if step > 0:
                    send(step - 1, d, cb).wait_recv()
                    part = part + r_buf[step - 1, d, cb].astype(F32)
                if step + 1 < n:
                    if step == 0:
                        s_buf[d, cb] = part.astype(BF16)
                    else:
                        r_buf[step - 1, d, cb] = part.astype(BF16)
                    send(step, d, cb).start()
                else:
                    finish(d, cb, part)
            if hook is not None:
                hook(step, cb)
            return 0

        lax.fori_loop(0, blocks, one_block, 0)

    def drain(cb, _):
        for step in range(n - 1):
            for d in range(2):
                send(step, d, cb).wait_send()
        return 0

    lax.fori_loop(0, blocks, drain, 0)


def ring_scratch(n, half, depth, block, blocks, n_u):
    return [
        pltpu.VMEM((2, 2, half, depth), BF16),
        pltpu.VMEM((2, depth, block), BF16),
        pltpu.VMEM((2, blocks, half, block), BF16),
        pltpu.VMEM((n - 1, 2, blocks, half, block), BF16),
        pltpu.SemaphoreType.DMA((2, 2, n_u)),
        pltpu.SemaphoreType.DMA((2,)),
        pltpu.SemaphoreType.DMA((n - 1, 2, blocks)),
        pltpu.SemaphoreType.DMA((n - 1, 2, blocks)),
    ]


def out_kernel(n, o_ref, w_ref, h_ref, gain_ref, r_ref, b_ref, h_buf, h_sem, u_buf, w_buf, s_buf, r_buf, u_sem, w_sem, send_sem, recv_sem):
    me, right, left = ring_place(n)
    shard, _ = r_ref.shape
    half = shard // 2
    block = w_buf.shape[2]
    load_h = pltpu.make_async_copy(h_ref.at[pl.ds(pl.multiple_of(me * shard, 16), shard), :], h_buf, h_sem)
    load_h.start()
    ring_barrier(right, left)

    def prepare(step):
        if step == n - 1:
            load_h.wait()

    def finish(d, cb, part):
        rows, cols = pl.ds(d * half, half), pl.ds(pl.multiple_of(cb * block, block), block)
        total = h_buf[rows, cols].astype(F32) + part.astype(BF16).astype(F32)
        r_ref[rows, cols] = total.astype(BF16)

    ring_matmul_scatter(n, me, (right, left), [o_ref], w_ref, u_buf, w_buf, s_buf, r_buf, u_sem, w_sem, send_sem, recv_sem, finish, prepare=prepare)
    gain = gain_ref[...]

    def norm_rows(i, _):
        rows = pl.ds(pl.multiple_of(i * 16, 16), 16)
        b_ref[rows, :] = rms_norm(r_ref[rows, :].astype(F32), gain)
        return 0

    lax.fori_loop(0, shard // 16, norm_rows, 0)


def out_project(n, mixed, w_out, hidden, gain):
    rows, depth = mixed.shape
    width = w_out.shape[1]
    shard = rows // n
    block = min(512, width // 2)
    blocks = width // block
    return pl.pallas_call(
        functools.partial(out_kernel, n),
        in_specs=[ANY, ANY, ANY, VMEM],
        out_specs=[VMEM, VMEM],
        out_shape=[jax.ShapeDtypeStruct((shard, width), BF16)] * 2,
        scratch_shapes=[pltpu.VMEM((shard, width), BF16), pltpu.SemaphoreType.DMA]
        + ring_scratch(n, shard // 2, depth, block, blocks, 1),
        compiler_params=pltpu.CompilerParams(collective_id=0, has_side_effects=True, vmem_limit_bytes=VMEM_LIMIT),
        cost_estimate=cost(2 * rows * depth * width * 5, 2 * (rows * depth + depth * width)),
    )(mixed, w_out, hidden, gain)


def gated(x, w_gate, w_up):
    gate = jnp.dot(x, w_gate, preferred_element_type=F32)
    up = jnp.dot(x, w_up, preferred_element_type=F32)
    return (jax.nn.silu(gate) * up).astype(BF16)


def gather_gate_kernel(n, pieces, b_ref, w_ref, all_ref, u_ref, w_buf, x_buf, u_buf, w_sem, x_sem, own_sem, u_sem, send_sem, recv_sem):
    me, right, left = ring_place(n)
    sides = (right, left)
    shard = b_ref.shape[0]
    half = shard // 2
    piece = half // pieces
    ff = u_ref.shape[1]
    tile = min(256, ff)
    tiles = ff // tile
    turns = [(a, j) for a in range(n) for j in range(pieces)]

    def w_copies(t):
        out = []
        for i in range(2):
            cols = pl.ds(pl.multiple_of(i * ff + t * tile, tile), tile)
            out.append(pltpu.make_async_copy(w_ref.at[:, cols], w_buf.at[:, cols], w_sem.at[t, i]))
        return out

    def rows_of(d, back, j):
        return pl.ds(pl.multiple_of(shard_of(me, d, back, n) * shard + d * half + j * piece, 16), piece)

    def own_rows(d, j):
        return b_ref.at[pl.ds(d * half + j * piece, piece), :]

    def hop(a, d, j):
        rows = rows_of(d, a, j)
        return pltpu.make_async_remote_copy(
            src_ref=own_rows(d, j) if a == 0 else all_ref.at[rows, :], dst_ref=all_ref.at[rows, :],
            send_sem=send_sem.at[a, d, j], recv_sem=recv_sem.at[a, d, j], device_id={'tp': sides[d]}, device_id_type=MESH)

    def arrival(a, d, j):
        rows = rows_of(d, a + 1, j)
        return pltpu.make_async_remote_copy(
            src_ref=all_ref.at[rows, :], dst_ref=all_ref.at[rows, :], send_sem=send_sem.at[a, d, j], recv_sem=recv_sem.at[a, d, j],
            device_id={'tp': sides[d]}, device_id_type=MESH)

    def x_copies(k):
        a, j = turns[k]
        return [pltpu.make_async_copy(
            own_rows(d, j) if a == 0 else all_ref.at[rows_of(d, a, j), :],
            x_buf.at[k % 2, pl.ds(d * piece, piece), :], x_sem.at[k % 2, d]) for d in range(2)]

    def keep_copies(k):
        a, j = turns[k]
        return [pltpu.make_async_copy(
            x_buf.at[k % 2, pl.ds(d * piece, piece), :], all_ref.at[rows_of(d, a, j), :], own_sem.at[j, d]) for d in range(2)]

    def u_copies(k):
        a, j = turns[k]
        return [pltpu.make_async_copy(
            u_buf.at[k % 2, pl.ds(d * piece, piece), :], u_ref.at[rows_of(d, a, j), :], u_sem.at[k % 2, d]) for d in range(2)]

    def start(copies):
        for c in copies:
            c.start()

    def wait(copies):
        for c in copies:
            c.wait()

    start(x_copies(0))

    def load_w(t, _):
        start(w_copies(t))
        return 0

    lax.fori_loop(0, tiles, load_w, 0)
    ring_barrier(right, left)
    for j in range(pieces):
        for d in range(2):
            hop(0, d, j).start()
    for k, (a, j) in enumerate(turns):
        if a > 0:
            for d in range(2):
                arrival(a - 1, d, j).wait_recv()
                if a + 1 < n:
                    hop(a, d, j).start()
            start(x_copies(k))
        wait(x_copies(k))
        if a == 0:
            start(keep_copies(k))
            if j > 0:
                wait(keep_copies(k - 1))
            if j + 1 < pieces:
                start(x_copies(k + 1))
        elif j == 0 and a == 1:
            wait(keep_copies(k - 1))
        if k >= 2:
            wait(u_copies(k - 2))

        def one_tile(t, _, k=k):
            if k == 0:
                wait(w_copies(t))
            at = pl.multiple_of(t * tile, tile)
            u_buf[k % 2, :, pl.ds(at, tile)] = gated(x_buf[k % 2], w_buf[:, pl.ds(at, tile)], w_buf[:, pl.ds(ff + at, tile)])
            return 0

        lax.fori_loop(0, tiles, one_tile, 0)
        start(u_copies(k))
    for k in range(len(turns) - 2, len(turns)):
        wait(u_copies(k))
    for a in range(n - 1):
        for j in range(pieces):
            for d in range(2):
                hop(a, d, j).wait_send()


def gather_gate(n, b, w):
    shard, depth = b.shape
    ff = w.shape[1] // 2
    tiles = ff // min(256, ff)
    pieces = 3
    piece = shard // 2 // pieces
    rows = shard * n
    return pl.pallas_call(
        functools.partial(gather_gate_kernel, n, pieces),
        in_specs=[ANY, ANY],
        out_specs=[ANY, ANY],
        out_shape=[jax.ShapeDtypeStruct((rows, depth), BF16), jax.ShapeDtypeStruct((rows, ff), BF16)],
        scratch_shapes=[
            pltpu.VMEM((depth, 2 * ff), BF16),
            pltpu.VMEM((2, 2 * piece, depth), BF16),
            pltpu.VMEM((2, 2 * piece, ff), BF16),
            pltpu.SemaphoreType.DMA((tiles, 2)),
            pltpu.SemaphoreType.DMA((2, 2)),
            pltpu.SemaphoreType.DMA((pieces, 2)),
            pltpu.SemaphoreType.DMA((2, 2)),
            pltpu.SemaphoreType.DMA((n - 1, 2, pieces)),
            pltpu.SemaphoreType.DMA((n - 1, 2, pieces)),
        ],
        compiler_params=pltpu.CompilerParams(collective_id=1, has_side_effects=True, vmem_limit_bytes=VMEM_LIMIT),
        cost_estimate=cost(4 * rows * depth * ff * 2, 2 * rows * depth + 2 * w.size),
    )(b, w)


def copy_kernel(x_ref, o_ref):
    o_ref[...] = x_ref[...]


def plain_copy(x, tile):
    spec = pl.BlockSpec((tile, x.shape[1]), lambda i: (i, 0))
    return pl.pallas_call(
        copy_kernel, grid=(x.shape[0] // tile,), in_specs=[spec], out_specs=spec, out_shape=jax.ShapeDtypeStruct(x.shape, x.dtype),
        cost_estimate=cost(1000, 4 * x.size))(x)


def part_cols(part, block, cb):
    return pl.ds(pl.multiple_of((2 * cb + part) * block, block), block)


def load_resid(r_ref, res_buf, res_sem, part, block, blocks):
    def copy(cb):
        return pltpu.make_async_copy(r_ref.at[:, part_cols(part, block, cb)], res_buf.at[cb], res_sem.at[cb])

    def begin(cb, _):
        copy(cb).start()
        return 0

    def end(cb, _):
        copy(cb).wait()
        return 0

    return lambda: lax.fori_loop(0, blocks, begin, 0), lambda: lax.fori_loop(0, blocks, end, 0)


def down_sum_kernel(n, x_ref, wb_ref, ua_ref, w_ref, r_ref, y_ref, ub_ref, wb_buf, x_buf, wb_sem, x_sem, ub_sem, res_buf, res_sem,
                    u_buf, w_buf, s_buf, r_buf, u_sem, w_sem, send_sem, recv_sem):
    me, right, left = ring_place(n)
    half = r_ref.shape[0] // 2
    blocks, _, block = res_buf.shape
    ff_a, ff = ua_ref.shape[1], ub_ref.shape[1]
    tile = min(256, ff)
    tiles = ff // tile
    begin, end = load_resid(r_ref, res_buf, res_sem, 0, block, blocks)

    def rows_of(d, step):
        return pl.ds(pl.multiple_of(shard_of(me, d, step + 1, n) * (2 * half) + d * half, 16), half)

    def x_copies(step):
        return [pltpu.make_async_copy(x_ref.at[rows_of(d, step), :], x_buf.at[pl.ds(d * half, half), :], x_sem.at[d]) for d in range(2)]

    def wb_copies(t):
        out = []
        for i in range(2):
            cols = pl.ds(pl.multiple_of(i * ff + t * tile, tile), tile)
            out.append(pltpu.make_async_copy(wb_ref.at[:, cols], wb_buf.at[:, cols], wb_sem.at[t, i]))
        return out

    def ub_copies(step):
        return [pltpu.make_async_copy(
            u_buf.at[step % 2, d, :, pl.ds(ff_a, ff)], ub_ref.at[rows_of(d, step), :], ub_sem.at[step % 2, d]) for d in range(2)]

    for c in x_copies(0):
        c.start()

    def load_wb(t, _):
        for c in wb_copies(t):
            c.start()
        return 0

    lax.fori_loop(0, tiles, load_wb, 0)
    begin()
    ring_barrier(right, left)

    def prepare(step):
        for c in x_copies(step):
            c.wait()
        if step >= 2:
            for c in ub_copies(step - 2):
                c.wait()

        def one_tile(t, _):
            if step == 0:
                for c in wb_copies(t):
                    c.wait()
            at = pl.multiple_of(t * tile, tile)
            act = gated(x_buf[...], wb_buf[:, pl.ds(at, tile)], wb_buf[:, pl.ds(ff + at, tile)])
            to = pl.ds(pl.multiple_of(ff_a + t * tile, tile), tile)
            for d in range(2):
                u_buf[step % 2, d, :, to] = act[d * half:(d + 1) * half, :]
            return 0

        lax.fori_loop(0, tiles, one_tile, 0)
        for c in ub_copies(step):
            c.start()
        if step + 1 < n:
            for c in x_copies(step + 1):
                c.start()
        else:
            end()

    def finish(d, cb, part):
        total = res_buf[cb, pl.ds(d * half, half), :].astype(F32) + part.astype(BF16).astype(F32)
        y_ref[d, cb] = total.astype(BF16)

    ring_matmul_scatter(n, me, (right, left), [ua_ref], w_ref, u_buf, w_buf, s_buf, r_buf, u_sem, w_sem, send_sem, recv_sem, finish,
                        prepare=prepare)
    for step in range(max(0, n - 2), n):
        for c in ub_copies(step):
            c.wait()


def down_kernel(n, ua_ref, ub_ref, w_ref, r_ref, first_ref, y_ref, res_buf, res_sem, own_sem, ag_send, ag_recv,
                u_buf, w_buf, s_buf, r_buf, u_sem, w_sem, send_sem, recv_sem):
    me, right, left = ring_place(n)
    sides = (right, left)
    shard = r_ref.shape[0]
    half = shard // 2
    blocks, _, block = res_buf.shape
    begin, end = load_resid(r_ref, res_buf, res_sem, 1, block, blocks)
    begin()
    ring_barrier(right, left)

    def place(d, back, part, cb):
        row = pl.multiple_of(shard_of(me, d, back, n) * shard + d * half, 16)
        return y_ref.at[pl.ds(row, half), part_cols(part, block, cb)]

    def own(d, part, cb):
        return first_ref.at[d, cb] if part == 0 else r_buf.at[n - 2, d, cb]

    def hop(a, d, part, cb):
        return pltpu.make_async_remote_copy(
            src_ref=own(d, part, cb) if a == 0 else place(d, a, part, cb), dst_ref=place(d, a, part, cb),
            send_sem=ag_send.at[a, d, part, cb], recv_sem=ag_recv.at[a, d, part, cb], device_id={'tp': sides[d]}, device_id_type=MESH)

    def arrival(a, d, part, cb):
        return pltpu.make_async_remote_copy(
            src_ref=place(d, a + 1, part, cb), dst_ref=place(d, a + 1, part, cb),
            send_sem=ag_send.at[a, d, part, cb], recv_sem=ag_recv.at[a, d, part, cb], device_id={'tp': sides[d]}, device_id_type=MESH)

    def keep(d, part, cb):
        return pltpu.make_async_copy(own(d, part, cb), place(d, 0, part, cb), own_sem.at[d, part, cb])

    def forward(a, part, cb):
        for d in range(2):
            arrival(a, d, part, cb).wait_recv()
            if a + 1 < n - 1:
                hop(a + 1, d, part, cb).start()

    def send_first(cb, _):
        for d in range(2):
            hop(0, d, 0, cb).start()
            keep(d, 0, cb).start()
        return 0

    lax.fori_loop(0, blocks, send_first, 0)

    def prepare(step):
        if step == n - 1:
            end()

    def finish(d, cb, part):
        total = res_buf[cb, pl.ds(d * half, half), :].astype(F32) + part.astype(BF16).astype(F32)
        r_buf[n - 2, d, cb] = total.astype(BF16)
        hop(0, d, 1, cb).start()
        keep(d, 1, cb).start()

    def hook(step, cb):
        if step > 0:
            forward(step - 1, 0, cb)

    ring_matmul_scatter(n, me, sides, [ua_ref, ub_ref], w_ref, u_buf, w_buf, s_buf, r_buf, u_sem, w_sem, send_sem, recv_sem, finish,
                        hook=hook, prepare=prepare)
    for a in range(n - 1):
        def last(cb, _, a=a):
            forward(a, 1, cb)
            return 0

        lax.fori_loop(0, blocks, last, 0)

    def drain(cb, _):
        for part in range(2):
            for d in range(2):
                keep(d, part, cb).wait()
                for a in range(n - 1):
                    hop(a, d, part, cb).wait_send()
        return 0

    lax.fori_loop(0, blocks, drain, 0)


def down_project(n, normed, w_b, act_a, w_first, w_second, resid, blocks):
    rows, width = normed.shape
    depth, part = w_first.shape
    ff = w_b.shape[1] // 2
    tiles = ff // min(256, ff)
    shard = rows // n
    block = part // blocks
    half = shard // 2
    resid_scratch = [pltpu.VMEM((blocks, shard, block), BF16), pltpu.SemaphoreType.DMA((blocks,))]
    params = dict(has_side_effects=True, vmem_limit_bytes=VMEM_LIMIT)
    first, act_b = pl.pallas_call(
        functools.partial(down_sum_kernel, n),
        in_specs=[ANY] * 5,
        out_specs=[VMEM, ANY],
        out_shape=[jax.ShapeDtypeStruct((2, blocks, half, block), BF16), jax.ShapeDtypeStruct((rows, ff), BF16)],
        scratch_shapes=[
            pltpu.VMEM(w_b.shape, BF16), pltpu.VMEM((shard, width), BF16),
            pltpu.SemaphoreType.DMA((tiles, 2)), pltpu.SemaphoreType.DMA((2,)), pltpu.SemaphoreType.DMA((2, 2)),
        ] + resid_scratch + ring_scratch(n, half, depth, block, blocks, 1),
        compiler_params=pltpu.CompilerParams(collective_id=2, **params),
        cost_estimate=cost(2 * rows * depth * part * 2, 2 * (rows * depth + depth * part)),
    )(normed, w_b, act_a, w_first, resid)
    ring = ring_scratch(n, half, depth, block, blocks, 2)
    return pl.pallas_call(
        functools.partial(down_kernel, n),
        in_specs=[ANY] * 5,
        out_specs=ANY,
        out_shape=jax.ShapeDtypeStruct((rows, 2 * part), BF16),
        scratch_shapes=resid_scratch + [
            pltpu.SemaphoreType.DMA((2, 2, blocks)),
            pltpu.SemaphoreType.DMA((n - 1, 2, 2, blocks)), pltpu.SemaphoreType.DMA((n - 1, 2, 2, blocks)),
        ] + ring,
        compiler_params=pltpu.CompilerParams(collective_id=3, **params),
        cost_estimate=cost(2 * rows * depth * part * 6, 2 * (rows * depth + depth * part)),
    )(act_a, act_b, w_second, resid, first)


def gather(shard, axis):
    return lax.all_gather(shard, GROUP_AXES, axis=axis, tiled=True)


def solution(mesh):
    n_tp = mesh.shape['tp']
    assert mesh.shape['cp'] == 2
    seq_spec = P(('dp', 'fsdp'), 'cp', None)
    pos_spec = P(('dp', 'fsdp'), 'cp')
    in_spec = P(GROUP_AXES, 'tp', None)
    out_spec = P('tp', None, GROUP_AXES)
    col_spec = P(GROUP_AXES, 'tp')
    row_spec = P('tp', GROUP_AXES)
    rep_spec = P(None)

    def layer_local(hidden, positions, attn_gain, w_query, w_key, w_value, w_out, mlp_gain, w_gate, w_up, w_down):
        n_seqs, tokens, d_model = hidden.shape
        heads, head = w_query.shape[1:]
        kv_heads = w_key.shape[1]
        rows = n_seqs * tokens
        local = w_query.shape[0]
        ff_a = w_gate.shape[1] * 10 // 14 // 256 * 256
        x = hidden.reshape(rows, d_model)

        w_qkv = jnp.concatenate([w.reshape(local, -1) for w in (w_query, w_key, w_value)], axis=1)
        full_qkv = gather(w_qkv, 0)
        full_out = gather(w_out.reshape(heads * head, -1), 1)
        full_a = gather(jnp.concatenate([w_gate[:, :ff_a], w_up[:, :ff_a]], axis=1), 0)
        full_b = gather(jnp.concatenate([w_gate[:, ff_a:], w_up[:, ff_a:]], axis=1), 0)
        down_half = w_down.shape[1] // 2
        full_down0 = gather(w_down[:, :down_half], 1)
        full_down1 = gather(w_down[:, down_half:], 1)

        normed = rms_norm(x.astype(F32), attn_gain)
        inv_freq = ROPE_THETA ** (-jnp.arange(0, head, 2, dtype=F32) / head)
        angles = positions.reshape(rows, 1).astype(F32) * inv_freq
        cos, sin = jnp.cos(angles), jnp.sin(angles)
        cos = jnp.concatenate([cos, cos], axis=1)
        sin = jnp.concatenate([-sin, sin], axis=1)

        q_width, kv_width = heads * head, 2 * kv_heads * head
        kv = project(normed, full_qkv, cos, sin, q_width // kv_width, kv_width, kv_heads, head)
        kv_peer = lax.ppermute(kv, 'cp', [(0, 1), (1, 0)])
        q = project(normed, full_qkv, cos, sin, 0, q_width, heads, head)
        mixed = attention(q, kv, kv_peer, n_seqs, kv_heads, heads // kv_heads, head)
        resid, normed_mlp = out_project(n_tp, mixed, full_out, x, mlp_gain.reshape(1, d_model))
        all_normed, act_a = gather_gate(n_tp, normed_mlp, full_a)
        y = down_project(n_tp, all_normed, full_b, act_a, full_down0, full_down1, resid, full_down0.shape[1] // down_half)
        y = plain_copy(y, rows // 16)
        return y.reshape(hidden.shape)

    return jax.shard_map(
        layer_local, mesh=mesh,
        in_specs=(seq_spec, pos_spec, rep_spec, in_spec, in_spec, in_spec, out_spec, rep_spec, col_spec, col_spec, row_spec),
        out_specs=seq_spec, check_vma=False)
```

```python
import functools
import math

import jax
import jax.numpy as jnp
from jax import lax
from jax.experimental import pallas as pl
from jax.experimental.pallas import tpu as pltpu
from jax.sharding import PartitionSpec as P


ROPE_THETA = 500000.0
NORM_EPS = 1e-5
GROUP_AXES = ('fsdp', 'cp')
VMEM_LIMIT = 62 * 1024 * 1024
F32 = jnp.float32
BF16 = jnp.bfloat16
MESH = pl.DeviceIdType.MESH
ANY = pl.BlockSpec(memory_space=pl.ANY)
VMEM = pl.BlockSpec(memory_space=pltpu.VMEM)


def rms_norm(hidden_f32, gain):
    mean_sq = jnp.mean(hidden_f32 * hidden_f32, axis=-1, keepdims=True)
    return (hidden_f32 * lax.rsqrt(mean_sq + NORM_EPS) * gain).astype(BF16)


def cost(flops, bytes_accessed):
    return pl.CostEstimate(flops=int(flops), bytes_accessed=int(bytes_accessed), transcendentals=0)


def proj_kernel(rope_heads, head, x_ref, w_ref, cos_ref, sin_ref, o_ref):
    acc = jnp.dot(x_ref[...], w_ref[...], preferred_element_type=F32)
    cos, sin = cos_ref[...], sin_ref[...]
    for i in range(acc.shape[1] // head):
        part = acc[:, i * head:(i + 1) * head]
        if i < rope_heads:
            part = part * cos + pltpu.roll(part, head // 2, 1) * sin
        o_ref[:, i * head:(i + 1) * head] = part.astype(BF16)


def project(x, w, cos, sin, col_block, width, rope_heads, head, tile=256):
    rows, depth = x.shape
    tile = math.gcd(tile, rows)
    return pl.pallas_call(
        functools.partial(proj_kernel, rope_heads, head),
        grid=(rows // tile,),
        in_specs=[
            pl.BlockSpec((tile, depth), lambda i: (i, 0)),
            pl.BlockSpec((depth, width), lambda i: (0, col_block)),
            pl.BlockSpec((tile, head), lambda i: (i, 0)),
            pl.BlockSpec((tile, head), lambda i: (i, 0)),
        ],
        out_specs=pl.BlockSpec((tile, width), lambda i: (i, 0)),
        out_shape=jax.ShapeDtypeStruct((rows, width), BF16),
        compiler_params=pltpu.CompilerParams(vmem_limit_bytes=VMEM_LIMIT),
        cost_estimate=cost(2 * rows * depth * width, 2 * (rows * depth + depth * width + rows * width)),
    )(x, w, cos, sin)


def attn_kernel(group, head, seg, q_ref, ko_ref, vo_ref, kp_ref, vp_ref, o_ref):
    c = lax.axis_index('cp')
    scale = head ** -0.5 * math.log2(math.e)

    def run(first_full, second_full):
        low, high = pl.ds(0, seg), pl.ds(seg, seg)
        own_low, own_high = (ko_ref, vo_ref, low), (ko_ref, vo_ref, high)
        tri = lax.broadcasted_iota(jnp.int32, (seg, seg), 0) >= lax.broadcasted_iota(jnp.int32, (seg, seg), 1)
        for g in range(group):
            cols = pl.ds(g * head, head)
            for rows, diag, full in ((low, own_low, first_full), (high, own_high, second_full)):
                q = q_ref[rows, cols]
                blocks = full + [diag]
                scores = []
                for k_ref, _, part in blocks:
                    scores.append(lax.dot_general(q, k_ref[part, :], (((1,), (1,)), ((), ())), preferred_element_type=F32))
                scores[-1] = jnp.where(tri, scores[-1], -jnp.inf)
                top = functools.reduce(jnp.maximum, [jnp.max(s, axis=-1, keepdims=True) for s in scores])
                total = jnp.zeros((seg, 1), F32)
                out = jnp.zeros((seg, head), F32)
                for s, (_, v_ref, part) in zip(scores, blocks):
                    p = jnp.exp2((s - top) * scale)
                    total = total + jnp.sum(p, axis=-1, keepdims=True)
                    out = out + jnp.dot(p.astype(BF16), v_ref[part, :], preferred_element_type=F32)
                o_ref[rows, cols] = (out / total).astype(BF16)

    low, high = pl.ds(0, seg), pl.ds(seg, seg)
    own_low, peer_low, peer_high = (ko_ref, vo_ref, low), (kp_ref, vp_ref, low), (kp_ref, vp_ref, high)

    @pl.when(c == 0)
    def _():
        run([], [own_low, peer_low, peer_high])

    @pl.when(c == 1)
    def _():
        run([peer_low], [peer_low, own_low])


def attention(q, kv_own, kv_peer, n_seqs, kv_heads, group, head):
    rows = q.shape[0]
    tokens = rows // n_seqs
    q_spec = pl.BlockSpec((tokens, group * head), lambda i, h: (i, h))
    k_spec = pl.BlockSpec((tokens, head), lambda i, h: (i, h))
    v_spec = pl.BlockSpec((tokens, head), lambda i, h: (i, kv_heads + h))
    return pl.pallas_call(
        functools.partial(attn_kernel, group, head, tokens // 2),
        grid=(n_seqs, kv_heads),
        in_specs=[q_spec, k_spec, v_spec, k_spec, v_spec],
        out_specs=q_spec,
        out_shape=jax.ShapeDtypeStruct(q.shape, BF16),
        compiler_params=pltpu.CompilerParams(vmem_limit_bytes=VMEM_LIMIT),
        cost_estimate=cost(10 * rows * tokens * kv_heads * group * head, 4 * q.size),
    )(q, kv_own, kv_own, kv_peer, kv_peer)


def ring_barrier(right, left):
    barrier = pltpu.get_barrier_semaphore()
    for neighbour in (right, left):
        pl.semaphore_signal(barrier, inc=1, device_id={'tp': neighbour}, device_id_type=MESH)
    pl.semaphore_wait(barrier, 2)


def ring_place(n):
    me = lax.axis_index('tp')
    return me, lax.rem(me + 1, n), lax.rem(me + n - 1, n)


def shard_of(me, direction, back, n):
    return lax.rem(me + (n - back if direction == 0 else back), n)


def ring_matmul_scatter(n, me, sides, u_refs, w_ref, u_buf, w_buf, s_buf, r_buf, u_sem, w_sem, send_sem, recv_sem, finish, hook=None, prepare=None):
    half = u_buf.shape[1] // 2
    block = w_buf.shape[2]
    blocks = w_ref.shape[1] // block

    def u_copies(step):
        copies = []
        for d in range(2):
            row = pl.multiple_of(shard_of(me, d, step + 1, n) * (2 * half) + d * half, 16)
            at = 0
            for i, u_ref in enumerate(u_refs):
                copies.append(pltpu.make_async_copy(
                    u_ref.at[pl.ds(row, half), :], u_buf.at[step % 2, pl.ds(d * half, half), pl.ds(at, u_ref.shape[1])], u_sem.at[step % 2, d, i]))
                at += u_ref.shape[1]
        return copies

    def w_copy(cb, slot):
        return pltpu.make_async_copy(w_ref.at[:, pl.ds(pl.multiple_of(cb * block, block), block)], w_buf.at[slot], w_sem.at[slot])

    def send(step, d, cb):
        src = s_buf.at[d, cb] if step == 0 else r_buf.at[step - 1, d, cb]
        return pltpu.make_async_remote_copy(
            src_ref=src, dst_ref=r_buf.at[step, d, cb], send_sem=send_sem.at[step, d, cb], recv_sem=recv_sem.at[step, d, cb],
            device_id={'tp': sides[d]}, device_id_type=MESH)

    for c in u_copies(0):
        c.start()
    w_copy(0, 0).start()
    for step in range(n):
        for c in u_copies(step):
            c.wait()
        if step + 1 < n:
            for c in u_copies(step + 1):
                c.start()
        if prepare is not None:
            prepare(step)

        def one_block(cb, _, step=step):
            slot = lax.rem(cb, 2)
            w_copy(cb, slot).wait()
            if step + 1 < n:
                w_copy(lax.rem(cb + 1, blocks), 1 - slot).start()
            else:
                @pl.when(cb + 1 < blocks)
                def _():
                    w_copy(cb + 1, 1 - slot).start()
            both = jnp.dot(u_buf[step % 2], w_buf[slot], preferred_element_type=F32)
            for d in range(2):
                part = both[d * half:(d + 1) * half]
                if step > 0:
                    send(step - 1, d, cb).wait_recv()
                    part = part + r_buf[step - 1, d, cb].astype(F32)
                if step + 1 < n:
                    if step == 0:
                        s_buf[d, cb] = part.astype(BF16)
                    else:
                        r_buf[step - 1, d, cb] = part.astype(BF16)
                    send(step, d, cb).start()
                else:
                    finish(d, cb, part)
            if hook is not None:
                hook(step, cb)
            return 0

        lax.fori_loop(0, blocks, one_block, 0)

    def drain(cb, _):
        for step in range(n - 1):
            for d in range(2):
                send(step, d, cb).wait_send()
        return 0

    lax.fori_loop(0, blocks, drain, 0)


def ring_scratch(n, half, depth, block, blocks, n_u):
    return [
        pltpu.VMEM((2, 2 * half, depth), BF16),
        pltpu.VMEM((2, depth, block), BF16),
        pltpu.VMEM((2, blocks, half, block), BF16),
        pltpu.VMEM((n - 1, 2, blocks, half, block), BF16),
        pltpu.SemaphoreType.DMA((2, 2, n_u)),
        pltpu.SemaphoreType.DMA((2,)),
        pltpu.SemaphoreType.DMA((n - 1, 2, blocks)),
        pltpu.SemaphoreType.DMA((n - 1, 2, blocks)),
    ]


def out_kernel(n, o_ref, w_ref, h_ref, gain_ref, r_ref, b_ref, h_buf, h_sem, u_buf, w_buf, s_buf, r_buf, u_sem, w_sem, send_sem, recv_sem):
    me, right, left = ring_place(n)
    shard, _ = r_ref.shape
    half = shard // 2
    block = w_buf.shape[2]
    load_h = pltpu.make_async_copy(h_ref.at[pl.ds(pl.multiple_of(me * shard, 16), shard), :], h_buf, h_sem)
    load_h.start()
    ring_barrier(right, left)

    def prepare(step):
        if step == n - 1:
            load_h.wait()

    def finish(d, cb, part):
        rows, cols = pl.ds(d * half, half), pl.ds(pl.multiple_of(cb * block, block), block)
        total = h_buf[rows, cols].astype(F32) + part.astype(BF16).astype(F32)
        r_ref[rows, cols] = total.astype(BF16)

    ring_matmul_scatter(n, me, (right, left), [o_ref], w_ref, u_buf, w_buf, s_buf, r_buf, u_sem, w_sem, send_sem, recv_sem, finish, prepare=prepare)
    gain = gain_ref[...]

    def norm_rows(i, _):
        rows = pl.ds(pl.multiple_of(i * 16, 16), 16)
        b_ref[rows, :] = rms_norm(r_ref[rows, :].astype(F32), gain)
        return 0

    lax.fori_loop(0, shard // 16, norm_rows, 0)


def out_project(n, mixed, w_out, hidden, gain):
    rows, depth = mixed.shape
    width = w_out.shape[1]
    shard = rows // n
    block = min(512, width // 2)
    blocks = width // block
    return pl.pallas_call(
        functools.partial(out_kernel, n),
        in_specs=[ANY, ANY, ANY, VMEM],
        out_specs=[VMEM, VMEM],
        out_shape=[jax.ShapeDtypeStruct((shard, width), BF16)] * 2,
        scratch_shapes=[pltpu.VMEM((shard, width), BF16), pltpu.SemaphoreType.DMA]
        + ring_scratch(n, shard // 2, depth, block, blocks, 1),
        compiler_params=pltpu.CompilerParams(collective_id=0, has_side_effects=True, vmem_limit_bytes=VMEM_LIMIT),
        cost_estimate=cost(2 * rows * depth * width * 5, 2 * (rows * depth + depth * width)),
    )(mixed, w_out, hidden, gain)


def gated(x, w_gate, w_up):
    gate = jnp.dot(x, w_gate, preferred_element_type=F32)
    up = jnp.dot(x, w_up, preferred_element_type=F32)
    return (jax.nn.silu(gate) * up).astype(BF16)


def gather_gate_kernel(n, pieces, b_ref, w_ref, all_ref, u_ref, w_buf, x_buf, u_buf, w_sem, x_sem, own_sem, u_sem, send_sem, recv_sem):
    me, right, left = ring_place(n)
    sides = (right, left)
    shard = b_ref.shape[0]
    half = shard // 2
    piece = half // pieces
    ff = u_ref.shape[1]
    tile = min(256, ff)
    tiles = ff // tile
    turns = [(a, j) for a in range(n) for j in range(pieces)]

    def w_copies(t):
        out = []
        for i in range(2):
            cols = pl.ds(pl.multiple_of(i * ff + t * tile, tile), tile)
            out.append(pltpu.make_async_copy(w_ref.at[:, cols], w_buf.at[:, cols], w_sem.at[t, i]))
        return out

    def rows_of(d, back, j):
        return pl.ds(pl.multiple_of(shard_of(me, d, back, n) * shard + d * half + j * piece, 16), piece)

    def own_rows(d, j):
        return b_ref.at[pl.ds(d * half + j * piece, piece), :]

    def hop(a, d, j):
        rows = rows_of(d, a, j)
        return pltpu.make_async_remote_copy(
            src_ref=own_rows(d, j) if a == 0 else all_ref.at[rows, :], dst_ref=all_ref.at[rows, :],
            send_sem=send_sem.at[a, d, j], recv_sem=recv_sem.at[a, d, j], device_id={'tp': sides[d]}, device_id_type=MESH)

    def arrival(a, d, j):
        rows = rows_of(d, a + 1, j)
        return pltpu.make_async_remote_copy(
            src_ref=all_ref.at[rows, :], dst_ref=all_ref.at[rows, :], send_sem=send_sem.at[a, d, j], recv_sem=recv_sem.at[a, d, j],
            device_id={'tp': sides[d]}, device_id_type=MESH)

    def x_copies(k):
        a, j = turns[k]
        return [pltpu.make_async_copy(
            own_rows(d, j) if a == 0 else all_ref.at[rows_of(d, a, j), :],
            x_buf.at[k % 2, pl.ds(d * piece, piece), :], x_sem.at[k % 2, d]) for d in range(2)]

    def keep_copies(k):
        a, j = turns[k]
        return [pltpu.make_async_copy(
            x_buf.at[k % 2, pl.ds(d * piece, piece), :], all_ref.at[rows_of(d, a, j), :], own_sem.at[j, d]) for d in range(2)]

    def u_copies(k):
        a, j = turns[k]
        return [pltpu.make_async_copy(
            u_buf.at[k % 2, pl.ds(d * piece, piece), :], u_ref.at[rows_of(d, a, j), :], u_sem.at[k % 2, d]) for d in range(2)]

    def start(copies):
        for c in copies:
            c.start()

    def wait(copies):
        for c in copies:
            c.wait()

    start(x_copies(0))

    def load_w(t, _):
        start(w_copies(t))
        return 0

    lax.fori_loop(0, tiles, load_w, 0)
    ring_barrier(right, left)
    for j in range(pieces):
        for d in range(2):
            hop(0, d, j).start()
    for k, (a, j) in enumerate(turns):
        if a > 0:
            for d in range(2):
                arrival(a - 1, d, j).wait_recv()
                if a + 1 < n:
                    hop(a, d, j).start()
            start(x_copies(k))
        wait(x_copies(k))
        if a == 0:
            start(keep_copies(k))
            if j > 0:
                wait(keep_copies(k - 1))
            if j + 1 < pieces:
                start(x_copies(k + 1))
        elif j == 0 and a == 1:
            wait(keep_copies(k - 1))
        if k >= 2:
            wait(u_copies(k - 2))

        def one_tile(t, _, k=k):
            if k == 0:
                wait(w_copies(t))
            at = pl.multiple_of(t * tile, tile)
            u_buf[k % 2, :, pl.ds(at, tile)] = gated(x_buf[k % 2], w_buf[:, pl.ds(at, tile)], w_buf[:, pl.ds(ff + at, tile)])
            return 0

        lax.fori_loop(0, tiles, one_tile, 0)
        start(u_copies(k))
    for k in range(len(turns) - 2, len(turns)):
        wait(u_copies(k))
    for a in range(n - 1):
        for j in range(pieces):
            for d in range(2):
                hop(a, d, j).wait_send()


def gather_gate(n, b, w):
    shard, depth = b.shape
    ff = w.shape[1] // 2
    tiles = ff // min(256, ff)
    pieces = 3
    piece = shard // 2 // pieces
    rows = shard * n
    return pl.pallas_call(
        functools.partial(gather_gate_kernel, n, pieces),
        in_specs=[ANY, ANY],
        out_specs=[ANY, ANY],
        out_shape=[jax.ShapeDtypeStruct((rows, depth), BF16), jax.ShapeDtypeStruct((rows, ff), BF16)],
        scratch_shapes=[
            pltpu.VMEM((depth, 2 * ff), BF16),
            pltpu.VMEM((2, 2 * piece, depth), BF16),
            pltpu.VMEM((2, 2 * piece, ff), BF16),
            pltpu.SemaphoreType.DMA((tiles, 2)),
            pltpu.SemaphoreType.DMA((2, 2)),
            pltpu.SemaphoreType.DMA((pieces, 2)),
            pltpu.SemaphoreType.DMA((2, 2)),
            pltpu.SemaphoreType.DMA((n - 1, 2, pieces)),
            pltpu.SemaphoreType.DMA((n - 1, 2, pieces)),
        ],
        compiler_params=pltpu.CompilerParams(collective_id=1, has_side_effects=True, vmem_limit_bytes=VMEM_LIMIT),
        cost_estimate=cost(4 * rows * depth * ff * 2, 2 * rows * depth + 2 * w.size),
    )(b, w)


def copy_kernel(x_ref, o_ref, buf, in_sem, out_sem):
    pieces, tile, _ = buf.shape

    def load(i):
        return pltpu.make_async_copy(x_ref.at[pl.ds(pl.multiple_of(i * tile, tile), tile), :], buf.at[i], in_sem.at[i])

    def store(i):
        return pltpu.make_async_copy(buf.at[i], o_ref.at[pl.ds(pl.multiple_of(i * tile, tile), tile), :], out_sem.at[i])

    def begin(i, _):
        load(i).start()
        return 0

    def turn(i, _):
        load(i).wait()
        store(i).start()
        return 0

    def end(i, _):
        store(i).wait()
        return 0

    for step in (begin, turn, end):
        lax.fori_loop(0, pieces, step, 0)


def plain_copy(x, pieces):
    rows, width = x.shape
    return pl.pallas_call(
        copy_kernel, in_specs=[ANY], out_specs=ANY, out_shape=jax.ShapeDtypeStruct(x.shape, x.dtype),
        scratch_shapes=[pltpu.VMEM((pieces, rows // pieces, width), x.dtype), pltpu.SemaphoreType.DMA((pieces,)), pltpu.SemaphoreType.DMA((pieces,))],
        compiler_params=pltpu.CompilerParams(vmem_limit_bytes=VMEM_LIMIT),
        cost_estimate=cost(1000, 4 * x.size))(x)


def part_cols(part, block, cb):
    return pl.ds(pl.multiple_of((2 * cb + part) * block, block), block)


def load_resid(r_ref, res_buf, res_sem, part, block, blocks):
    def copy(cb):
        return pltpu.make_async_copy(r_ref.at[:, part_cols(part, block, cb)], res_buf.at[cb], res_sem.at[cb])

    def begin(cb, _):
        copy(cb).start()
        return 0

    def end(cb, _):
        copy(cb).wait()
        return 0

    return lambda: lax.fori_loop(0, blocks, begin, 0), lambda: lax.fori_loop(0, blocks, end, 0)


def down_sum_kernel(n, x_ref, wb_ref, ua_ref, w_ref, r_ref, y_ref, ub_ref, wb_buf, x_buf, wb_sem, x_sem, ub_sem, res_buf, res_sem,
                    u_buf, w_buf, s_buf, r_buf, u_sem, w_sem, send_sem, recv_sem):
    me, right, left = ring_place(n)
    half = r_ref.shape[0] // 2
    blocks, _, block = res_buf.shape
    ff_a, ff = ua_ref.shape[1], ub_ref.shape[1]
    tile = min(256, ff)
    tiles = ff // tile
    begin, end = load_resid(r_ref, res_buf, res_sem, 0, block, blocks)

    def rows_of(d, step):
        return pl.ds(pl.multiple_of(shard_of(me, d, step + 1, n) * (2 * half) + d * half, 16), half)

    def x_copies(step):
        return [pltpu.make_async_copy(x_ref.at[rows_of(d, step), :], x_buf.at[pl.ds(d * half, half), :], x_sem.at[d]) for d in range(2)]

    def wb_copies(t):
        out = []
        for i in range(2):
            cols = pl.ds(pl.multiple_of(i * ff + t * tile, tile), tile)
            out.append(pltpu.make_async_copy(wb_ref.at[:, cols], wb_buf.at[:, cols], wb_sem.at[t, i]))
        return out

    def ub_copies(step):
        return [pltpu.make_async_copy(
            u_buf.at[step % 2, pl.ds(d * half, half), pl.ds(ff_a, ff)], ub_ref.at[rows_of(d, step), :], ub_sem.at[step % 2, d]) for d in range(2)]

    for c in x_copies(0):
        c.start()

    def load_wb(t, _):
        for c in wb_copies(t):
            c.start()
        return 0

    lax.fori_loop(0, tiles, load_wb, 0)
    begin()
    ring_barrier(right, left)

    def prepare(step):
        for c in x_copies(step):
            c.wait()
        if step >= 2:
            for c in ub_copies(step - 2):
                c.wait()

        def one_tile(t, _):
            if step == 0:
                for c in wb_copies(t):
                    c.wait()
            at = pl.multiple_of(t * tile, tile)
            to = pl.ds(pl.multiple_of(ff_a + t * tile, tile), tile)
            u_buf[step % 2, :, to] = gated(x_buf[...], wb_buf[:, pl.ds(at, tile)], wb_buf[:, pl.ds(ff + at, tile)])
            return 0

        lax.fori_loop(0, tiles, one_tile, 0)
        for c in ub_copies(step):
            c.start()
        if step + 1 < n:
            for c in x_copies(step + 1):
                c.start()
        else:
            end()

    def finish(d, cb, part):
        total = res_buf[cb, pl.ds(d * half, half), :].astype(F32) + part.astype(BF16).astype(F32)
        y_ref[d, cb] = total.astype(BF16)

    ring_matmul_scatter(n, me, (right, left), [ua_ref], w_ref, u_buf, w_buf, s_buf, r_buf, u_sem, w_sem, send_sem, recv_sem, finish,
                        prepare=prepare)
    for step in range(max(0, n - 2), n):
        for c in ub_copies(step):
            c.wait()


def down_kernel(n, ua_ref, ub_ref, w_ref, r_ref, first_ref, y_ref, res_buf, res_sem, own_sem, ag_send, ag_recv,
                u_buf, w_buf, s_buf, r_buf, u_sem, w_sem, send_sem, recv_sem):
    me, right, left = ring_place(n)
    sides = (right, left)
    shard = r_ref.shape[0]
    half = shard // 2
    blocks, _, block = res_buf.shape
    begin, end = load_resid(r_ref, res_buf, res_sem, 1, block, blocks)
    begin()
    ring_barrier(right, left)

    def place(d, back, part, cb):
        row = pl.multiple_of(shard_of(me, d, back, n) * shard + d * half, 16)
        return y_ref.at[pl.ds(row, half), part_cols(part, block, cb)]

    def own(d, part, cb):
        return first_ref.at[d, cb] if part == 0 else r_buf.at[n - 2, d, cb]

    def hop(a, d, part, cb):
        return pltpu.make_async_remote_copy(
            src_ref=own(d, part, cb) if a == 0 else place(d, a, part, cb), dst_ref=place(d, a, part, cb),
            send_sem=ag_send.at[a, d, part, cb], recv_sem=ag_recv.at[a, d, part, cb], device_id={'tp': sides[d]}, device_id_type=MESH)

    def arrival(a, d, part, cb):
        return pltpu.make_async_remote_copy(
            src_ref=place(d, a + 1, part, cb), dst_ref=place(d, a + 1, part, cb),
            send_sem=ag_send.at[a, d, part, cb], recv_sem=ag_recv.at[a, d, part, cb], device_id={'tp': sides[d]}, device_id_type=MESH)

    def keep(d, part, cb):
        return pltpu.make_async_copy(own(d, part, cb), place(d, 0, part, cb), own_sem.at[d, part, cb])

    def forward(a, part, cb):
        for d in range(2):
            arrival(a, d, part, cb).wait_recv()
            if a + 1 < n - 1:
                hop(a + 1, d, part, cb).start()

    def send_first(cb, _):
        for d in range(2):
            hop(0, d, 0, cb).start()
            keep(d, 0, cb).start()
        return 0

    lax.fori_loop(0, blocks, send_first, 0)

    def prepare(step):
        if step == n - 1:
            end()

    def finish(d, cb, part):
        total = res_buf[cb, pl.ds(d * half, half), :].astype(F32) + part.astype(BF16).astype(F32)
        r_buf[n - 2, d, cb] = total.astype(BF16)
        hop(0, d, 1, cb).start()
        keep(d, 1, cb).start()

    def hook(step, cb):
        if step > 0:
            forward(step - 1, 0, cb)

    ring_matmul_scatter(n, me, sides, [ua_ref, ub_ref], w_ref, u_buf, w_buf, s_buf, r_buf, u_sem, w_sem, send_sem, recv_sem, finish,
                        hook=hook, prepare=prepare)
    for a in range(n - 1):
        def last(cb, _, a=a):
            forward(a, 1, cb)
            return 0

        lax.fori_loop(0, blocks, last, 0)

    def drain(cb, _):
        for part in range(2):
            for d in range(2):
                keep(d, part, cb).wait()
                for a in range(n - 1):
                    hop(a, d, part, cb).wait_send()
        return 0

    lax.fori_loop(0, blocks, drain, 0)


def down_project(n, normed, w_b, act_a, w_first, w_second, resid, blocks):
    rows, width = normed.shape
    depth, part = w_first.shape
    ff = w_b.shape[1] // 2
    tiles = ff // min(256, ff)
    shard = rows // n
    block = part // blocks
    half = shard // 2
    resid_scratch = [pltpu.VMEM((blocks, shard, block), BF16), pltpu.SemaphoreType.DMA((blocks,))]
    params = dict(has_side_effects=True, vmem_limit_bytes=VMEM_LIMIT)
    first, act_b = pl.pallas_call(
        functools.partial(down_sum_kernel, n),
        in_specs=[ANY] * 5,
        out_specs=[VMEM, ANY],
        out_shape=[jax.ShapeDtypeStruct((2, blocks, half, block), BF16), jax.ShapeDtypeStruct((rows, ff), BF16)],
        scratch_shapes=[
            pltpu.VMEM(w_b.shape, BF16), pltpu.VMEM((shard, width), BF16),
            pltpu.SemaphoreType.DMA((tiles, 2)), pltpu.SemaphoreType.DMA((2,)), pltpu.SemaphoreType.DMA((2, 2)),
        ] + resid_scratch + ring_scratch(n, half, depth, block, blocks, 1),
        compiler_params=pltpu.CompilerParams(collective_id=2, **params),
        cost_estimate=cost(2 * rows * depth * part * 2, 2 * (rows * depth + depth * part)),
    )(normed, w_b, act_a, w_first, resid)
    ring = ring_scratch(n, half, depth, block, blocks, 2)
    return pl.pallas_call(
        functools.partial(down_kernel, n),
        in_specs=[ANY] * 5,
        out_specs=ANY,
        out_shape=jax.ShapeDtypeStruct((rows, 2 * part), BF16),
        scratch_shapes=resid_scratch + [
            pltpu.SemaphoreType.DMA((2, 2, blocks)),
            pltpu.SemaphoreType.DMA((n - 1, 2, 2, blocks)), pltpu.SemaphoreType.DMA((n - 1, 2, 2, blocks)),
        ] + ring,
        compiler_params=pltpu.CompilerParams(collective_id=3, **params),
        cost_estimate=cost(2 * rows * depth * part * 6, 2 * (rows * depth + depth * part)),
    )(act_a, act_b, w_second, resid, first)


def gather(shard, axis):
    return lax.all_gather(shard, GROUP_AXES, axis=axis, tiled=True)


def solution(mesh):
    n_tp = mesh.shape['tp']
    assert mesh.shape['cp'] == 2
    seq_spec = P(('dp', 'fsdp'), 'cp', None)
    pos_spec = P(('dp', 'fsdp'), 'cp')
    in_spec = P(GROUP_AXES, 'tp', None)
    out_spec = P('tp', None, GROUP_AXES)
    col_spec = P(GROUP_AXES, 'tp')
    row_spec = P('tp', GROUP_AXES)
    rep_spec = P(None)

    def layer_local(hidden, positions, attn_gain, w_query, w_key, w_value, w_out, mlp_gain, w_gate, w_up, w_down):
        n_seqs, tokens, d_model = hidden.shape
        heads, head = w_query.shape[1:]
        kv_heads = w_key.shape[1]
        rows = n_seqs * tokens
        local = w_query.shape[0]
        ff_a = w_gate.shape[1] * 10 // 14 // 256 * 256
        x = hidden.reshape(rows, d_model)

        w_qkv = jnp.concatenate([w.reshape(local, -1) for w in (w_query, w_key, w_value)], axis=1)
        full_qkv = gather(w_qkv, 0)
        full_out = gather(w_out.reshape(heads * head, -1), 1)
        full_a = gather(jnp.concatenate([w_gate[:, :ff_a], w_up[:, :ff_a]], axis=1), 0)
        full_b = gather(jnp.concatenate([w_gate[:, ff_a:], w_up[:, ff_a:]], axis=1), 0)
        down_half = w_down.shape[1] // 2
        full_down0 = gather(w_down[:, :down_half], 1)
        full_down1 = gather(w_down[:, down_half:], 1)

        normed = rms_norm(x.astype(F32), attn_gain)
        inv_freq = ROPE_THETA ** (-jnp.arange(0, head, 2, dtype=F32) / head)
        angles = positions.reshape(rows, 1).astype(F32) * inv_freq
        cos, sin = jnp.cos(angles), jnp.sin(angles)
        cos = jnp.concatenate([cos, cos], axis=1)
        sin = jnp.concatenate([-sin, sin], axis=1)

        q_width, kv_width = heads * head, 2 * kv_heads * head
        kv = project(normed, full_qkv, cos, sin, q_width // kv_width, kv_width, kv_heads, head)
        kv_peer = lax.ppermute(kv, 'cp', [(0, 1), (1, 0)])
        q = project(normed, full_qkv, cos, sin, 0, q_width, heads, head)
        mixed = attention(q, kv, kv_peer, n_seqs, kv_heads, heads // kv_heads, head)
        resid, normed_mlp = out_project(n_tp, mixed, full_out, x, mlp_gain.reshape(1, d_model))
        all_normed, act_a = gather_gate(n_tp, normed_mlp, full_a)
        y = down_project(n_tp, all_normed, full_b, act_a, full_down0, full_down1, resid, full_down0.shape[1] // down_half)
        y = plain_copy(y, 24)
        return y.reshape(hidden.shape)

    return jax.shard_map(
        layer_local, mesh=mesh,
        in_specs=(seq_spec, pos_spec, rep_spec, in_spec, in_spec, in_spec, out_spec, rep_spec, col_spec, col_spec, row_spec),
        out_specs=seq_spec, check_vma=False)
```
